32 devices in a mesh: row: 4 (over x, core), col: 8 (over z, y).
Axes of the slice: x: 2, y: 2, z: 4, core: 2. Of those that a mesh axis runs over, the one named last changes fastest.
Arguments:
- tokens: bfloat16 [16384, 1024], P(('row', 'col')), may hold values from -6 to 6
- expert_ids: int32 [16384, 1], P(('row', 'col')), may hold values from 0 to 31; in each aligned block of 512 rows (0 to 511, 512 to 1023, ...) at most 32 rows name the same one
- gate_prob: float32 [16384], P(('row', 'col')), may hold values from 0.25 to 1
- norm_gain: float32 [1024], replicated, may hold values from 0.1 to 1.9
- weight_in: bfloat16 [32, 1024, 4096], P(('row', 'col')), may hold values from -0.1875 to 0.1875
- weight_out: bfloat16 [32, 4096, 1024], P(('row', 'col')), may hold values from -0.09375 to 0.09375
Outputs:
- mixed: bfloat16 [16384, 1024], P(('row', 'col'))
- routed: int32 [32], P(('row', 'col'))
The draws below stay inside these ranges and needn't reach their ends.
Inputs may be any that keep to these rules, and one draw needn't show every extreme that they name: `expert_ids`: among the 512 tokens of one device no expert is chosen more than 32 times; some expert is chosen exactly 32 times by some device's tokens.
All inputs are finite; a program needn't handle non-finite values.
Results may differ from the reference program's by a relative error of at most 0.001.
The reference program's roundings to bfloat16 on the way (of `normed`, `slots`, `hidden` and `answers`) count: a program that leaves them out, or rounds other values in their place, can miss the bound.
Values may be sent and summed in bfloat16 or wider, within the bound.
A program may use at most 64 MiB of HBM per device.

```python
import math
import jax
import jax.numpy as jnp
import numpy as np
from jax import lax

D = 1024
FF = 4096
TOK_DEV = 512
EXPERTS = 32
CAP = 32
TOKENS = 16384
DEVICES = 32


def draw_tokens(key, part):
    base_key = jax.random.fold_in(key, 11)
    value_key, sparse_key, choose_key = jax.random.split(base_key, 3)
    values = jnp.clip(jax.random.normal(value_key, (TOKENS, D), jnp.float32), -6.0, 6.0)
    sparse_rows = jax.random.randint(sparse_key, (TOKENS,), 0, 64) == 0
    chosen = jax.random.randint(choose_key, (TOKENS // TOK_DEV,), 0, TOK_DEV)
    position = jnp.arange(TOKENS, dtype=jnp.int32)
    block_index = position // TOK_DEV
    forced_rows = position % TOK_DEV == chosen[block_index]
    kept_rows = jnp.logical_not(jnp.logical_or(sparse_rows, forced_rows)).astype(jnp.float32)
    return (values * kept_rows[:, None]).astype(jnp.bfloat16)


def levels(key, dims, cuts, low, high):
    level, own = 1.0, jax.random.fold_in(key, 6)
    for dim, parts in cuts:
        steps = jnp.exp(jax.random.uniform(jax.random.fold_in(own, dim), (parts,), jnp.float32, low / len(cuts), high / len(cuts)))
        level = level * jnp.repeat(steps, dims[dim] // parts).reshape([-1 if axis == dim else 1 for axis in range(len(dims))])
    return level


def routed_block(own_key, own, number, rows, number_of, top, reach, lean):
    order = jax.random.permutation(own_key, number_of)
    heavy_load, usual = portions_of(number_of, rows * top, reach, lean, True), portions_of(number_of, rows * top, reach, lean, False)
    places = jnp.arange(number_of)

    def named(tallies, offset_by):
        used = int((tallies > 0).sum())
        fixed = max(1, used // 4)
        moved = fixed + (places - fixed + offset_by * (used - fixed)) % max(1, number_of - fixed)
        return jnp.zeros((number_of,), jnp.int32).at[order[jnp.where(places < fixed, places, moved)]].set(jnp.asarray(tallies, jnp.int32))

    tallies = jnp.where(number % 4 == 0, named(heavy_load, number // 4), named(usual, number - number // 4 - 1))
    mixed = jax.random.permutation(jax.random.fold_in(own, 3), number_of)
    donor, sink = mixed[0:number_of // 2 * 2:2], mixed[1:number_of // 2 * 2:2]
    room = jnp.minimum(tallies[donor] - 1, reach - tallies[sink]) // 2
    room = jnp.where((donor == order[0]) | (sink == order[0]) | (tallies[sink] == 0), 0, jnp.maximum(room, 0))
    moved = jax.random.randint(jax.random.fold_in(own, 4), (number_of // 2,), 0, 1 << 20) % (room + 1)
    tallies = tallies.at[donor].add(-moved).at[sink].add(moved)
    labels = jnp.searchsorted(jnp.cumsum(tallies), jnp.arange(rows * top), side="right").astype(jnp.int32)
    table = labels.reshape(top, rows).T
    table = table[jax.random.permutation(jax.random.fold_in(own, 1), rows)]
    offset_by = jax.random.randint(jax.random.fold_in(own, 2), (rows, 1), 0, top)
    return jnp.take_along_axis(table, (jnp.arange(top)[None, :] + offset_by) % top, axis=1)


def portions_of(number_of, total, reach, skew, full):
    weights = [(1 << 20) // math.isqrt(rank ** skew) + 1 for rank in range(1, number_of + 1)]
    largest = reach if full else min(reach, max(-(-total // number_of), total * weights[0] // sum(weights)))
    least = 1 if total - largest >= number_of - 1 else 0
    holding, rest = [largest] + [least] * (number_of - 1), total - largest - least * (number_of - 1)
    while rest > 0:
        candidates = [i for i in range(1, number_of) if holding[i] < largest] or [i for i in range(1, number_of) if holding[i] < reach]
        pool, budget = sum([weights[i] for i in candidates]), rest
        for i in candidates:
            more = min(reach - holding[i], max(1, budget * weights[i] // pool), rest)
            holding[i] = holding[i] + more
            rest = rest - more
    return np.array(holding)


def normal_values(stream_key, dims, width, reach, shards=(), held_as=jnp.bfloat16):
    entries = jax.random.normal(stream_key, dims, jnp.float32) * width
    if len(shards) > 0:
        entries = levels(stream_key, dims, shards, -0.22, 0.18) * entries
    return jnp.clip(entries, min=-reach, max=reach).astype(held_as)


def setup_inputs(seed: int = 0) -> dict:
    seeds = jax.random.split(jax.random.key(seed), 7)
    tokens = draw_tokens(jax.random.fold_in(seeds[6], 71), 0)
    expert_ids_keys = jax.random.split(jax.random.fold_in(seeds[1], 1), TOKENS // TOK_DEV)
    expert_ids_turns = jax.random.permutation(jax.random.fold_in(seeds[1], 3), TOKENS // TOK_DEV)
    expert_ids = jax.vmap(lambda own, number: routed_block(jax.random.fold_in(seeds[1], 2), own, number, TOK_DEV, EXPERTS, 1, CAP, 2))(expert_ids_keys, expert_ids_turns).reshape((TOKENS, 1))
    gate_prob = jnp.clip(0.25 + 0.75 * jax.random.uniform(seeds[2], (TOKENS,), jnp.float32) ** levels(seeds[2], (TOKENS,), ((0, 32),), -0.2, 0.2), 0.25, 1.0)
    norm_gain = jnp.clip(1.0 + 0.18 * jax.random.normal(seeds[3], (D,), jnp.float32), 0.1, 1.9)
    weight_in = normal_values(seeds[4], (EXPERTS, D, FF), D ** -0.5, 0.1875, ((0, 32),))
    weight_out = normal_values(seeds[5], (EXPERTS, FF, D), FF ** -0.5, 0.09375, ((0, 32),))
    return {"tokens": tokens, "expert_ids": expert_ids, "gate_prob": gate_prob, "norm_gain": norm_gain, "weight_in": weight_in, "weight_out": weight_out}


def slot_rank(block_ids):
    count = block_ids.shape[0]
    same = block_ids[:, None] == block_ids[None, :]
    earlier = jnp.arange(count, dtype=jnp.int32)[None, :] < jnp.arange(count, dtype=jnp.int32)[:, None]
    return lax.optimization_barrier(jnp.sum((same & earlier).astype(jnp.int32), axis=1)).astype(jnp.int32)

def expert_ffn(pieces):
    slab, first, second = pieces
    hidden = jnp.maximum(jnp.dot(slab, first, preferred_element_type=jnp.float32), 0.0).astype(jnp.bfloat16)
    return jnp.dot(hidden, second, preferred_element_type=jnp.float32).astype(jnp.bfloat16)

def reference(tokens, expert_ids, gate_prob, norm_gain, weight_in, weight_out):
    flat_ids = expert_ids[:, 0].astype(jnp.int32)
    within = jax.vmap(slot_rank)(flat_ids.reshape(DEVICES, TOK_DEV)).reshape(-1)
    source = (jnp.arange(TOKENS, dtype=jnp.int32) // TOK_DEV).astype(jnp.int32)
    placed = ((flat_ids * DEVICES + source) * CAP + within).astype(jnp.int32)
    wide = tokens.astype(jnp.float32)
    scale = lax.rsqrt(lax.optimization_barrier(jnp.mean(wide * wide, axis=1, keepdims=True)) + 1e-06)
    normed = (wide * scale * norm_gain[None, :]).astype(jnp.bfloat16)
    slots = jnp.zeros((EXPERTS * DEVICES * CAP, D), jnp.bfloat16).at[placed].set(normed)
    slots = slots.reshape(EXPERTS, DEVICES * CAP, D)
    answers = lax.map(expert_ffn, (slots, weight_in, weight_out))
    back = answers.reshape(EXPERTS * DEVICES * CAP, D)[placed]
    mixed = (wide + gate_prob[:, None] * back.astype(jnp.float32)).astype(jnp.bfloat16)
    routed = lax.optimization_barrier(jnp.sum((flat_ids[:, None] == jnp.arange(EXPERTS, dtype=jnp.int32)[None, :]).astype(jnp.int32), axis=0))
    return (mixed, routed)
```

```python
import functools

import jax
import jax.numpy as jnp
from jax import lax
from jax.experimental import pallas as pl
from jax.experimental.pallas import tpu as pltpu
from jax.sharding import PartitionSpec as P

MESH = pl.DeviceIdType.MESH


def bit_xor(a, b, size):
    out, unit = 0, 1
    while unit < size:
        out = out + lax.rem(lax.div(a, unit) + lax.div(b, unit), 2) * unit
        unit *= 2
    return out


def kernel(
    rows, cols, cap, groups, ff_tile, out_tile,
    tokens_ref, ids_row_ref, gain_ref, first_hbm, second_hbm,
    back_ref, routed_ref,
    first, second, normed, outgoing, received, answers, returned, hidden, total,
    counts, counts_in, placed_col,
    weight_sem, send_sem, recv_sem, ret_sem, count_sem,
):
    n = rows * cols
    tok_rows, width = tokens_ref.shape
    lanes = counts.shape[1]
    per = n // groups
    span = per * cap
    my_row, my_col = lax.axis_index("row"), lax.axis_index("col")
    me = my_row * cols + my_col

    def turn(step):
        if groups % 2:
            return step
        return lax.rem(step, 2) * (groups // 2) + lax.div(step, 2)

    def partner(place):
        q = n - 1 - place
        return (
            bit_xor(my_row, lax.rem(q, rows), rows),
            bit_xor(my_col, lax.div(q, rows), cols),
        )

    barrier = pltpu.get_barrier_semaphore()

    @pl.loop(0, n - 1)
    def _(place):
        pl.semaphore_signal(barrier, inc=1, device_id=partner(place), device_id_type=MESH)

    load_first = pltpu.make_async_copy(first_hbm.at[0], first, weight_sem.at[0])
    load_second = pltpu.make_async_copy(second_hbm.at[0], second, weight_sem.at[1])
    load_first.start()
    load_second.start()

    def slot_of(ids, within):
        offset = jnp.bitwise_xor(ids, me)
        q = (offset % cols) * rows + offset // cols
        return (n - 1 - q) * cap + within

    ids_row = ids_row_ref[...]
    at_row = lax.broadcasted_iota(jnp.int32, (tok_rows, tok_rows), 0)
    at_col = lax.broadcasted_iota(jnp.int32, (tok_rows, tok_rows), 1)
    hot_row = lax.broadcasted_iota(jnp.int32, (lanes, tok_rows), 0) == ids_row
    before = jnp.where(at_row < at_col, 1.0, 0.0).astype(jnp.bfloat16)
    earlier = jnp.dot(
        jnp.where(hot_row, 1.0, 0.0).astype(jnp.bfloat16), before, preferred_element_type=jnp.float32
    )
    within_row = jnp.sum(jnp.where(hot_row, earlier, 0.0), axis=0, keepdims=True)
    placed_row = slot_of(ids_row, within_row.astype(jnp.int32))

    wide = tokens_ref[...].astype(jnp.float32)
    scale = lax.rsqrt(jnp.mean(wide * wide, axis=1, keepdims=True) + 1e-06)
    normed[...] = (wide * scale * gain_ref[...]).astype(jnp.bfloat16)

    def as_blocks(values):
        return values.reshape(per, cap, width).astype(jnp.bfloat16)

    def as_rows(ref, g):
        blocks = ref[pl.ds(g * per, per)]
        if cap % 16 == 0:
            return blocks.reshape(span, width)
        return blocks.astype(jnp.float32).reshape(span, width).astype(jnp.bfloat16)

    def exchange(source, target, sem, out_sem, g):
        @pl.loop(0, per)
        def _(i):
            place = g * per + i

            @pl.when(place < n - 1)
            def _():
                pltpu.make_async_remote_copy(
                    src_ref=source.at[place],
                    dst_ref=target.at[place],
                    send_sem=out_sem,
                    recv_sem=sem.at[g],
                    device_id=partner(place),
                    device_id_type=MESH,
                ).start()

            @pl.when(place == n - 1)
            def _():
                pltpu.make_async_copy(source.at[n - 1], target.at[n - 1], sem.at[g]).start()

    def wait_group(target, sem, g):
        whole = target.at[pl.ds(g * per, per)]
        pltpu.make_async_copy(whole, whole, sem.at[g]).wait()

    @pl.loop(0, groups)
    def _(step):
        g = turn(step)
        slot = lax.broadcasted_iota(jnp.int32, (span, tok_rows), 0) + g * span
        table = jnp.where(slot == placed_row, 1.0, 0.0).astype(jnp.bfloat16)
        outgoing[pl.ds(g * per, per)] = as_blocks(
            jnp.dot(table, normed[...], preferred_element_type=jnp.float32)
        )

        @pl.when(step == 0)
        def _():
            pl.semaphore_wait(barrier, n - 1)

        exchange(outgoing, received, recv_sem, send_sem.at[0], g)

    counts[...] = lax.dot_general(
        jnp.ones((8, tok_rows), jnp.bfloat16),
        jnp.where(hot_row, 1.0, 0.0).astype(jnp.bfloat16),
        (((1,), (1,)), ((), ())),
        preferred_element_type=jnp.float32,
    )[0:1]
    turned = jnp.where(at_row == at_col, placed_row.astype(jnp.float32), 0.0)
    placed_col[...] = jnp.sum(turned, axis=1, keepdims=True).astype(jnp.int32)
    total[...] = jnp.zeros_like(total)

    @pl.loop(0, n - 1)
    def _(place):
        pltpu.make_async_remote_copy(
            src_ref=counts,
            dst_ref=counts_in.at[place],
            send_sem=send_sem.at[2],
            recv_sem=count_sem,
            device_id=partner(place),
            device_id_type=MESH,
        ).start()

    load_first.wait()
    load_second.wait()

    @pl.loop(0, groups)
    def _(step):
        g = turn(lax.rem(step + groups - 1, groups))
        wait_group(received, recv_sem, g)
        slab = as_rows(received, g)

        @pl.loop(0, first.shape[1] // ff_tile)
        def _(i):
            part = pl.ds(pl.multiple_of(i * ff_tile, ff_tile), ff_tile)
            grown = jnp.dot(slab, first[:, part], preferred_element_type=jnp.float32)
            hidden[:, part] = jnp.maximum(grown, 0.0).astype(jnp.bfloat16)

        @pl.loop(0, width // out_tile)
        def _(i):
            part = pl.ds(pl.multiple_of(i * out_tile, out_tile), out_tile)
            made = jnp.dot(hidden[...], second[:, part], preferred_element_type=jnp.float32)
            answers[pl.ds(g * per, per), :, part] = made.reshape(per, cap, out_tile).astype(
                jnp.bfloat16
            )

        exchange(answers, returned, ret_sem, send_sem.at[1], g)

    arrived = counts_in.at[pl.ds(0, n - 1)]
    pltpu.make_async_copy(arrived, arrived, count_sem).wait()
    sums = jnp.sum(counts_in[pl.ds(0, n - 1)], axis=0) + counts[...]
    mine = lax.broadcasted_iota(jnp.int32, (1, lanes), 1) == me
    routed_ref[0] = jnp.sum(jnp.where(mine, sums, 0.0)).astype(jnp.int32)

    @pl.loop(0, groups)
    def _(step):
        g = turn(lax.rem(step + groups - 1, groups))
        wait_group(returned, ret_sem, g)
        slot = lax.broadcasted_iota(jnp.int32, (tok_rows, span), 1) + g * span
        table = jnp.where(slot == placed_col[...], 1.0, 0.0).astype(jnp.bfloat16)
        total[...] += jnp.dot(table, as_rows(returned, g), preferred_element_type=jnp.float32)

    back_ref[...] = total[...].astype(jnp.bfloat16)

    sent = outgoing.at[pl.ds(0, n - 1)]
    pltpu.make_async_copy(sent, sent, send_sem.at[0]).wait()
    pltpu.make_async_copy(sent, sent, send_sem.at[1]).wait()
    pltpu.make_async_copy(arrived, arrived, send_sem.at[2]).wait()


def flipped(a, mask, size):
    out, unit = 0, 1
    while unit < size:
        bit = lax.rem(lax.div(a, unit), 2)
        out = out + ((1 - bit) if (mask // unit) % 2 else bit) * unit
        unit *= 2
    return out


def packed_kernel(
    rows, cols, low, cap, keep, parts, ff_tile, out_tile,
    tokens_ref, ids_row_ref, gate_row_ref, gain_ref, first_hbm, second_hbm,
    mixed_ref, routed_ref, over_ref,
    first, second, normed, packed, packed_in, slots, slots_in, answers, answers_in,
    back, back_in, hidden, total, counts, counts_far, counts_in,
    index_row, index_col, placed_col, gate_col,
    weight_sem, send_sem, far_sem, near_sem, answer_sem, back_sem, count_sem,
):
    n = rows * cols
    planes = cols // low
    per = n // planes
    span = per * cap
    tok_rows, width = tokens_ref.shape
    wide_part = width // parts
    lanes = counts.shape[1]
    my_row, my_col = lax.axis_index("row"), lax.axis_index("col")
    me = my_row * cols + my_col
    row_at = [flipped(my_row, c, rows) for c in range(rows)]
    low_at = [flipped(lax.rem(my_col, low), c, low) for c in range(low)]
    plane_at = [flipped(lax.div(my_col, low), c, planes) * low for c in range(planes)]
    far = list(range(planes - 1, 0, -1))

    def device(k, j):
        return (row_at[j % rows], plane_at[k] + low_at[j // rows])

    def send(source, target, out_sem, sem, where):
        pltpu.make_async_remote_copy(
            src_ref=source, dst_ref=target, send_sem=out_sem, recv_sem=sem,
            device_id=where, device_id_type=MESH,
        ).start()

    def wait(ref, sem):
        pltpu.make_async_copy(ref, ref, sem).wait()

    barrier = pltpu.get_barrier_semaphore()
    for k in range(planes):
        for j in range(per):
            if k or j:
                pl.semaphore_signal(barrier, inc=1, device_id=device(k, j), device_id_type=MESH)

    load_first = pltpu.make_async_copy(first_hbm.at[0], first, weight_sem.at[0])
    load_second = pltpu.make_async_copy(second_hbm.at[0], second, weight_sem.at[1])
    load_first.start()
    load_second.start()

    def place_of(ids):
        offset = jnp.bitwise_xor(ids, me)
        return (offset % cols) // low, offset // cols + rows * (offset % low)

    def ones_at(condition):
        return jnp.where(condition, 1.0, 0.0).astype(jnp.bfloat16)

    ids_row = ids_row_ref[...]
    at_row = lax.broadcasted_iota(jnp.int32, (tok_rows, tok_rows), 0)
    at_col = lax.broadcasted_iota(jnp.int32, (tok_rows, tok_rows), 1)
    hot = lax.broadcasted_iota(jnp.int32, (lanes, tok_rows), 0) == ids_row
    hot_bf = ones_at(hot)
    earlier = jnp.dot(hot_bf, ones_at(at_row < at_col), preferred_element_type=jnp.float32)
    within = jnp.sum(jnp.where(hot, earlier, 0.0), axis=0, keepdims=True)
    plane_e, near_e = place_of(lax.broadcasted_iota(jnp.int32, (lanes, 1), 0))
    plane_t, near_t = place_of(ids_row)
    count_e = jnp.sum(jnp.where(hot, 1.0, 0.0), axis=1, keepdims=True)
    sooner = (plane_e == plane_t) & (near_e < near_t)
    ahead = jnp.sum(jnp.where(sooner, count_e, 0.0), axis=0, keepdims=True)
    start = jnp.where(plane_t == 0, near_t * cap, ahead.astype(jnp.int32))
    placed_row = plane_t * span + start + within.astype(jnp.int32)

    wide = tokens_ref[...].astype(jnp.float32)
    scale = lax.rsqrt(jnp.mean(wide * wide, axis=1, keepdims=True) + 1e-06)
    normed[...] = (wide * scale * gain_ref[...]).astype(jnp.bfloat16)

    tally = lax.dot_general(
        jnp.ones((8, tok_rows), jnp.bfloat16), hot_bf,
        (((1,), (1,)), ((), ())), preferred_element_type=jnp.float32,
    )[0:1]
    lane = lax.broadcasted_iota(jnp.int32, (1, lanes), 1)
    plane_l, _ = place_of(lane)
    over = jnp.zeros((1, 1), jnp.float32)
    for k in far:
        held = jnp.sum(jnp.where(plane_l == k, tally, 0.0), axis=1, keepdims=True)
        over = over + jnp.where(held > keep, 1.0, 0.0)
    counts[...] = tally + jnp.where(lane == n, over, 0.0)

    def columns(h):
        return pl.ds(h * wide_part, wide_part)

    def gather_from(k, size):
        slot = lax.broadcasted_iota(jnp.int32, (size, tok_rows), 0) + k * span
        return ones_at(slot == placed_row)

    def pack(k):
        table = gather_from(k, keep)
        for h in range(parts):
            packed[k, h] = jnp.dot(
                table, normed[:, columns(h)], preferred_element_type=jnp.float32
            ).astype(jnp.bfloat16)

    def send_far(k):
        for h in range(parts):
            send(packed.at[k, h], packed_in.at[k, h], send_sem.at[0], far_sem.at[k, h], device(k, 0))

    def send_near(source, target, out_sem, sem, k, h):
        for j in range(1, per):
            block = pl.ds(j * cap, cap)
            send(
                source.at[k, h, block], target.at[k, h, block], out_sem, sem.at[k, h], device(0, j)
            )

    def wait_near(target, sem, k, h):
        wait(target.at[k, h, pl.ds(cap, span - cap)], sem.at[k, h])

    def fill(k, h, values):
        made = values.astype(jnp.bfloat16)
        slots_in[k, h, 0:cap] = made[0:cap]
        slots[k, h] = made
        send_near(slots, slots_in, send_sem.at[1], near_sem, k, h)

    pack(far[0])
    pl.semaphore_wait(barrier, n - 1)
    for k in far:
        send(counts, counts_far.at[k], send_sem.at[4], count_sem.at[0], device(k, 0))
    send_far(far[0])
    table = gather_from(0, span)
    for h in range(parts):
        fill(0, h, jnp.dot(table, normed[:, columns(h)], preferred_element_type=jnp.float32))
    for k in far[1:]:
        pack(k)
        send_far(k)
    for k in range(planes):
        for j in range(1, per):
            send(
                counts, counts_in.at[k * (per - 1) + j - 1], send_sem.at[5], count_sem.at[1],
                device(k, j),
            )

    def to_column(row, size):
        there = lax.broadcasted_iota(jnp.int32, (size, size), 0)
        here = lax.broadcasted_iota(jnp.int32, (size, size), 1)
        return jnp.sum(jnp.where(there == here, row, 0.0), axis=1, keepdims=True)

    placed_col[...] = to_column(placed_row.astype(jnp.float32), tok_rows).astype(jnp.int32)
    gate_col[...] = to_column(gate_row_ref[...], tok_rows)

    wait(counts_far.at[pl.ds(1, planes - 1)], count_sem.at[0])
    expert = lax.broadcasted_iota(jnp.int32, (lanes, span), 0)
    plane_s, near_s = place_of(expert)
    here = (plane_s == 0) & (expert < n)
    slot = lax.broadcasted_iota(jnp.int32, (lanes, span), 1)
    at_block = ones_at(here & (near_s == slot // cap))
    before_block = ones_at(here & (near_s < slot // cap))
    slot_row = lax.broadcasted_iota(jnp.int32, (1, span), 1)
    rank = (slot_row % cap).astype(jnp.float32)
    for k in far:
        tall = jnp.broadcast_to(counts_far[k], (8, lanes)).astype(jnp.bfloat16)
        held = jnp.dot(tall, at_block, preferred_element_type=jnp.float32)[0:1]
        begin = jnp.dot(tall, before_block, preferred_element_type=jnp.float32)[0:1]
        index = jnp.where(rank < held, begin + rank, -1.0)
        index_row[k] = index.astype(jnp.int32)
        index_col[k] = to_column(index, span).astype(jnp.int32)

    load_first.wait()
    load_second.wait()

    def relay(k, h):
        wait(packed_in.at[k, h], far_sem.at[k, h])
        slot = lax.broadcasted_iota(jnp.int32, (span, keep), 1)
        table = ones_at(slot == index_col[k])
        fill(k, h, jnp.dot(table, packed_in[k, h], preferred_element_type=jnp.float32))

    def expert_step(k):
        for h in range(parts):
            wait_near(slots_in, near_sem, k, h)

        @pl.loop(0, first.shape[1] // ff_tile)
        def _(i):
            part = pl.ds(pl.multiple_of(i * ff_tile, ff_tile), ff_tile)
            grown = jnp.dot(slots_in[k, 0], first[columns(0), part], preferred_element_type=jnp.float32)
            for h in range(1, parts):
                grown += jnp.dot(
                    slots_in[k, h], first[columns(h), part], preferred_element_type=jnp.float32
                )
            hidden[:, part] = jnp.maximum(grown, 0.0).astype(jnp.bfloat16)

        for h in range(parts):

            @pl.loop(0, wide_part // out_tile)
            def _(i):
                at = pl.multiple_of(i * out_tile, out_tile)
                part = pl.ds(pl.multiple_of(h * wide_part + i * out_tile, out_tile), out_tile)
                made = jnp.dot(hidden[...], second[:, part], preferred_element_type=jnp.float32)
                made = made.astype(jnp.bfloat16)
                answers[k, h, :, pl.ds(at, out_tile)] = made
                answers_in[k, h, 0:cap, pl.ds(at, out_tile)] = made[0:cap]

            send_near(answers, answers_in, send_sem.at[2], answer_sem, k, h)

    def give_back(k, h):
        wait_near(answers_in, answer_sem, k, h)
        slot = lax.broadcasted_iota(jnp.int32, (keep, span), 0)
        table = ones_at(slot == index_row[k])
        back[k, h] = jnp.dot(
            table, answers_in[k, h], preferred_element_type=jnp.float32
        ).astype(jnp.bfloat16)
        send(back.at[k, h], back_in.at[k, h], send_sem.at[3], back_sem.at[k, h], device(k, 0))

    def picked(k, h):
        size = keep if k else span
        if k:
            wait(back_in.at[k, h], back_sem.at[k, h])
        else:
            wait_near(answers_in, answer_sem, 0, h)
        source = back_in if k else answers_in
        slot = lax.broadcasted_iota(jnp.int32, (tok_rows, size), 1) + k * span
        table = ones_at(slot == placed_col[...])
        return jnp.dot(table, source[k, h], preferred_element_type=jnp.float32)

    expert_step(0)
    for h in range(parts):
        relay(far[0], h)
    for i, k in enumerate(far):
        expert_step(k)
        later = far[i + 1] if i + 1 < len(far) else None
        if later is not None:
            relay(later, 0)
        for h in range(parts):
            give_back(k, h)
        if later is not None:
            for h in range(1, parts):
                relay(later, h)

    wait(counts_in, count_sem.at[1])
    sums = jnp.sum(counts_in[...], axis=0) + counts[...]
    sums += jnp.sum(counts_far[pl.ds(1, planes - 1)], axis=0)
    routed_ref[0] = jnp.sum(jnp.where(lane == me, sums, 0.0)).astype(jnp.int32)
    over_ref[0] = jnp.sum(jnp.where(lane == n, sums, 0.0)).astype(jnp.int32)

    for h in range(parts):
        total[h] = picked(0, h)
    for k in far[:-1]:
        for h in range(parts):
            total[h] += picked(k, h)
    for h in range(parts):
        found = total[h] + picked(far[-1], h)
        kept = tokens_ref[:, columns(h)].astype(jnp.float32)
        mixed_ref[:, columns(h)] = (kept + gate_col[...] * found).astype(jnp.bfloat16)

    wait(packed.at[pl.ds(1, planes - 1)], send_sem.at[0])
    wait(slots.at[:, :, pl.ds(cap, span - cap)], send_sem.at[1])
    wait(answers.at[:, :, pl.ds(cap, span - cap)], send_sem.at[2])
    wait(back.at[pl.ds(1, planes - 1)], send_sem.at[3])
    wait(counts_far.at[pl.ds(1, planes - 1)], send_sem.at[4])
    wait(counts_in, send_sem.at[5])


def packed_layer(rows, cols, tokens, expert_ids, gate_prob, norm_gain, weight_in, weight_out):
    tok_rows, width = tokens.shape
    hidden_width = weight_in.shape[2]
    n = rows * cols
    low = min(2, cols)
    planes = cols // low
    per = n // planes
    cap = 2 * tok_rows // n
    span = per * cap
    keep = 3 * span // 4
    parts = 2
    part = width // parts
    lanes = -(-(n + 1) // 128) * 128
    vmem = pl.BlockSpec(memory_space=pltpu.VMEM)
    smem = pl.BlockSpec(memory_space=pltpu.SMEM)
    hbm = pl.BlockSpec(memory_space=pl.ANY)
    tight = pltpu.VMEM((planes, parts, keep, part), jnp.bfloat16)
    loose = pltpu.VMEM((planes, parts, span, part), jnp.bfloat16)
    each = pltpu.SemaphoreType.DMA((planes, parts))
    return pl.pallas_call(
        functools.partial(
            packed_kernel, rows, cols, low, cap, keep, parts,
            min(512, hidden_width), min(256, part),
        ),
        out_shape=(
            jax.ShapeDtypeStruct((tok_rows, width), jnp.bfloat16),
            jax.ShapeDtypeStruct((1,), jnp.int32),
            jax.ShapeDtypeStruct((1,), jnp.int32),
        ),
        in_specs=[vmem, vmem, vmem, vmem, hbm, hbm],
        out_specs=(vmem, smem, smem),
        scratch_shapes=[
            pltpu.VMEM((width, hidden_width), jnp.bfloat16),
            pltpu.VMEM((hidden_width, width), jnp.bfloat16),
            pltpu.VMEM((tok_rows, width), jnp.bfloat16),
            tight, tight, loose, loose, loose, loose, tight, tight,
            pltpu.VMEM((span, hidden_width), jnp.bfloat16),
            pltpu.VMEM((parts, tok_rows, part), jnp.float32),
            pltpu.VMEM((1, lanes), jnp.float32),
            pltpu.VMEM((planes, 1, lanes), jnp.float32),
            pltpu.VMEM((planes * (per - 1), 1, lanes), jnp.float32),
            pltpu.VMEM((planes, 1, span), jnp.int32),
            pltpu.VMEM((planes, span, 1), jnp.int32),
            pltpu.VMEM((tok_rows, 1), jnp.int32),
            pltpu.VMEM((tok_rows, 1), jnp.float32),
            pltpu.SemaphoreType.DMA((2,)),
            pltpu.SemaphoreType.DMA((6,)),
            each, each, each, each,
            pltpu.SemaphoreType.DMA((2,)),
        ],
        compiler_params=pltpu.CompilerParams(
            collective_id=0, has_side_effects=True, vmem_limit_bytes=56 * 1024 * 1024
        ),
    )(
        tokens,
        expert_ids.reshape(1, tok_rows),
        gate_prob.reshape(1, tok_rows),
        norm_gain.reshape(1, width),
        weight_in,
        weight_out,
    )


def slotted_layer(rows, cols, tokens, expert_ids, gate_prob, norm_gain, weight_in, weight_out):
    tok_rows, width = tokens.shape
    hidden_width = weight_in.shape[2]
    n = rows * cols
    cap = 2 * tok_rows // n
    lanes = -(-n // 128) * 128
    per = max(1, min(n, 256 // cap))
    groups = n // per
    vmem = pl.BlockSpec(memory_space=pltpu.VMEM)
    hbm = pl.BlockSpec(memory_space=pl.ANY)
    block = pltpu.VMEM((n, cap, width), jnp.bfloat16)
    back, routed = pl.pallas_call(
        functools.partial(kernel, rows, cols, cap, groups, min(512, hidden_width), min(256, width)),
        out_shape=(
            jax.ShapeDtypeStruct((tok_rows, width), jnp.bfloat16),
            jax.ShapeDtypeStruct((1,), jnp.int32),
        ),
        in_specs=[vmem, vmem, vmem, hbm, hbm],
        out_specs=(vmem, pl.BlockSpec(memory_space=pltpu.SMEM)),
        scratch_shapes=[
            pltpu.VMEM((width, hidden_width), jnp.bfloat16),
            pltpu.VMEM((hidden_width, width), jnp.bfloat16),
            pltpu.VMEM((tok_rows, width), jnp.bfloat16),
            block, block, block, block,
            pltpu.VMEM((per * cap, hidden_width), jnp.bfloat16),
            pltpu.VMEM((tok_rows, width), jnp.float32),
            pltpu.VMEM((1, lanes), jnp.float32),
            pltpu.VMEM((n, 1, lanes), jnp.float32),
            pltpu.VMEM((tok_rows, 1), jnp.int32),
            pltpu.SemaphoreType.DMA((2,)),
            pltpu.SemaphoreType.DMA((3,)),
            pltpu.SemaphoreType.DMA((groups,)),
            pltpu.SemaphoreType.DMA((groups,)),
            pltpu.SemaphoreType.DMA,
        ],
        compiler_params=pltpu.CompilerParams(
            collective_id=1, has_side_effects=True, vmem_limit_bytes=56 * 1024 * 1024
        ),
    )(
        tokens,
        expert_ids.reshape(1, tok_rows),
        norm_gain.reshape(1, width),
        weight_in,
        weight_out,
    )
    wide = tokens.astype(jnp.float32)
    mixed = (wide + gate_prob[:, None] * back.astype(jnp.float32)).astype(jnp.bfloat16)
    return mixed


def on_device(rows, cols, *args):
    mixed, routed, over = packed_layer(rows, cols, *args)
    mixed = lax.cond(
        over[0] > 0, lambda given, *all_args: slotted_layer(rows, cols, *all_args),
        lambda given, *all_args: given, mixed, *args,
    )
    return (mixed, routed)


def solution(mesh):
    return jax.shard_map(
        functools.partial(on_device, mesh.shape["row"], mesh.shape["col"]),
        mesh=mesh,
        in_specs=(
            P(("row", "col"), None),
            P(("row", "col"), None),
            P(("row", "col")),
            P(),
            P(("row", "col"), None, None),
            P(("row", "col"), None, None),
        ),
        out_specs=(P(("row", "col"), None), P(("row", "col"))),
        check_vma=False,
    )
```

```python
import functools

import jax
import jax.numpy as jnp
from jax import lax
from jax.experimental import pallas as pl
from jax.experimental.pallas import tpu as pltpu
from jax.sharding import PartitionSpec as P

MESH = pl.DeviceIdType.MESH


def bit_xor(a, b, size):
    out, unit = 0, 1
    while unit < size:
        out = out + lax.rem(lax.div(a, unit) + lax.div(b, unit), 2) * unit
        unit *= 2
    return out


def kernel(
    rows, cols, cap, groups, ff_tile, out_tile,
    tokens_ref, ids_row_ref, gain_ref, first_hbm, second_hbm,
    back_ref, routed_ref,
    first, second, normed, outgoing, received, answers, returned, hidden, total,
    counts, counts_in, placed_col,
    weight_sem, send_sem, recv_sem, ret_sem, count_sem,
):
    n = rows * cols
    tok_rows, width = tokens_ref.shape
    lanes = counts.shape[1]
    per = n // groups
    span = per * cap
    my_row, my_col = lax.axis_index("row"), lax.axis_index("col")
    me = my_row * cols + my_col

    def turn(step):
        if groups % 2:
            return step
        return lax.rem(step, 2) * (groups // 2) + lax.div(step, 2)

    def partner(place):
        q = n - 1 - place
        return (
            bit_xor(my_row, lax.rem(q, rows), rows),
            bit_xor(my_col, lax.div(q, rows), cols),
        )

    barrier = pltpu.get_barrier_semaphore()

    @pl.loop(0, n - 1)
    def _(place):
        pl.semaphore_signal(barrier, inc=1, device_id=partner(place), device_id_type=MESH)

    load_first = pltpu.make_async_copy(first_hbm.at[0], first, weight_sem.at[0])
    load_second = pltpu.make_async_copy(second_hbm.at[0], second, weight_sem.at[1])
    load_first.start()
    load_second.start()

    def slot_of(ids, within):
        offset = jnp.bitwise_xor(ids, me)
        q = (offset % cols) * rows + offset // cols
        return (n - 1 - q) * cap + within

    ids_row = ids_row_ref[...]
    at_row = lax.broadcasted_iota(jnp.int32, (tok_rows, tok_rows), 0)
    at_col = lax.broadcasted_iota(jnp.int32, (tok_rows, tok_rows), 1)
    hot_row = lax.broadcasted_iota(jnp.int32, (lanes, tok_rows), 0) == ids_row
    before = jnp.where(at_row < at_col, 1.0, 0.0).astype(jnp.bfloat16)
    earlier = jnp.dot(
        jnp.where(hot_row, 1.0, 0.0).astype(jnp.bfloat16), before, preferred_element_type=jnp.float32
    )
    within_row = jnp.sum(jnp.where(hot_row, earlier, 0.0), axis=0, keepdims=True)
    placed_row = slot_of(ids_row, within_row.astype(jnp.int32))

    wide = tokens_ref[...].astype(jnp.float32)
    scale = lax.rsqrt(jnp.mean(wide * wide, axis=1, keepdims=True) + 1e-06)
    normed[...] = (wide * scale * gain_ref[...]).astype(jnp.bfloat16)

    def as_blocks(values):
        return values.reshape(per, cap, width).astype(jnp.bfloat16)

    def as_rows(ref, g):
        blocks = ref[pl.ds(g * per, per)]
        if cap % 16 == 0:
            return blocks.reshape(span, width)
        return blocks.astype(jnp.float32).reshape(span, width).astype(jnp.bfloat16)

    def exchange(source, target, sem, out_sem, g):
        @pl.loop(0, per)
        def _(i):
            place = g * per + i

            @pl.when(place < n - 1)
            def _():
                pltpu.make_async_remote_copy(
                    src_ref=source.at[place],
                    dst_ref=target.at[place],
                    send_sem=out_sem,
                    recv_sem=sem.at[g],
                    device_id=partner(place),
                    device_id_type=MESH,
                ).start()

            @pl.when(place == n - 1)
            def _():
                pltpu.make_async_copy(source.at[n - 1], target.at[n - 1], sem.at[g]).start()

    def wait_group(target, sem, g):
        whole = target.at[pl.ds(g * per, per)]
        pltpu.make_async_copy(whole, whole, sem.at[g]).wait()

    @pl.loop(0, groups)
    def _(step):
        g = turn(step)
        slot = lax.broadcasted_iota(jnp.int32, (span, tok_rows), 0) + g * span
        table = jnp.where(slot == placed_row, 1.0, 0.0).astype(jnp.bfloat16)
        outgoing[pl.ds(g * per, per)] = as_blocks(
            jnp.dot(table, normed[...], preferred_element_type=jnp.float32)
        )

        @pl.when(step == 0)
        def _():
            pl.semaphore_wait(barrier, n - 1)

        exchange(outgoing, received, recv_sem, send_sem.at[0], g)

    counts[...] = lax.dot_general(
        jnp.ones((8, tok_rows), jnp.bfloat16),
        jnp.where(hot_row, 1.0, 0.0).astype(jnp.bfloat16),
        (((1,), (1,)), ((), ())),
        preferred_element_type=jnp.float32,
    )[0:1]
    turned = jnp.where(at_row == at_col, placed_row.astype(jnp.float32), 0.0)
    placed_col[...] = jnp.sum(turned, axis=1, keepdims=True).astype(jnp.int32)
    total[...] = jnp.zeros_like(total)

    @pl.loop(0, n - 1)
    def _(place):
        pltpu.make_async_remote_copy(
            src_ref=counts,
            dst_ref=counts_in.at[place],
            send_sem=send_sem.at[2],
            recv_sem=count_sem,
            device_id=partner(place),
            device_id_type=MESH,
        ).start()

    load_first.wait()
    load_second.wait()

    @pl.loop(0, groups)
    def _(step):
        g = turn(lax.rem(step + groups - 1, groups))
        wait_group(received, recv_sem, g)
        slab = as_rows(received, g)

        @pl.loop(0, first.shape[1] // ff_tile)
        def _(i):
            part = pl.ds(pl.multiple_of(i * ff_tile, ff_tile), ff_tile)
            grown = jnp.dot(slab, first[:, part], preferred_element_type=jnp.float32)
            hidden[:, part] = jnp.maximum(grown, 0.0).astype(jnp.bfloat16)

        @pl.loop(0, width // out_tile)
        def _(i):
            part = pl.ds(pl.multiple_of(i * out_tile, out_tile), out_tile)
            made = jnp.dot(hidden[...], second[:, part], preferred_element_type=jnp.float32)
            answers[pl.ds(g * per, per), :, part] = made.reshape(per, cap, out_tile).astype(
                jnp.bfloat16
            )

        exchange(answers, returned, ret_sem, send_sem.at[1], g)

    arrived = counts_in.at[pl.ds(0, n - 1)]
    pltpu.make_async_copy(arrived, arrived, count_sem).wait()
    sums = jnp.sum(counts_in[pl.ds(0, n - 1)], axis=0) + counts[...]
    mine = lax.broadcasted_iota(jnp.int32, (1, lanes), 1) == me
    routed_ref[0] = jnp.sum(jnp.where(mine, sums, 0.0)).astype(jnp.int32)

    @pl.loop(0, groups)
    def _(step):
        g = turn(lax.rem(step + groups - 1, groups))
        wait_group(returned, ret_sem, g)
        slot = lax.broadcasted_iota(jnp.int32, (tok_rows, span), 1) + g * span
        table = jnp.where(slot == placed_col[...], 1.0, 0.0).astype(jnp.bfloat16)
        total[...] += jnp.dot(table, as_rows(returned, g), preferred_element_type=jnp.float32)

    back_ref[...] = total[...].astype(jnp.bfloat16)

    sent = outgoing.at[pl.ds(0, n - 1)]
    pltpu.make_async_copy(sent, sent, send_sem.at[0]).wait()
    pltpu.make_async_copy(sent, sent, send_sem.at[1]).wait()
    pltpu.make_async_copy(arrived, arrived, send_sem.at[2]).wait()


def flipped(a, mask, size):
    out, unit = 0, 1
    while unit < size:
        bit = lax.rem(lax.div(a, unit), 2)
        out = out + ((1 - bit) if (mask // unit) % 2 else bit) * unit
        unit *= 2
    return out


def packed_kernel(
    rows, cols, low, cap, keep, parts, ff_tile, out_tile,
    tokens_ref, ids_row_ref, gate_row_ref, gain_ref, first_hbm, second_hbm,
    mixed_ref, routed_ref, over_ref,
    first, second, normed, packed, packed_in, slots, slots_in, answers, answers_in,
    back, back_in, hidden, total, counts, counts_far, counts_in,
    index_row, index_col, placed_col, gate_col,
    weight_sem, send_sem, far_sem, near_sem, answer_sem, back_sem, count_sem,
):
    n = rows * cols
    planes = cols // low
    per = n // planes
    span = per * cap
    tok_rows, width = tokens_ref.shape
    wide_part = width // parts
    lanes = counts.shape[1]
    my_row, my_col = lax.axis_index("row"), lax.axis_index("col")
    me = my_row * cols + my_col
    row_at = [flipped(my_row, c, rows) for c in range(rows)]
    low_at = [flipped(lax.rem(my_col, low), c, low) for c in range(low)]
    plane_at = [flipped(lax.div(my_col, low), c, planes) * low for c in range(planes)]
    far = list(range(planes - 1, 0, -1))
    half = planes // 2
    sent = [planes - 1 - k for i in range(half) for k in (i, i + half)][: planes - 1]
    if planes % 2:
        sent = far

    def device(k, j):
        return (row_at[j % rows], plane_at[k] + low_at[j // rows])

    def send(source, target, out_sem, sem, where):
        pltpu.make_async_remote_copy(
            src_ref=source, dst_ref=target, send_sem=out_sem, recv_sem=sem,
            device_id=where, device_id_type=MESH,
        ).start()

    def wait(ref, sem, name="wait_last"):
        with jax.named_scope(name):
            pltpu.make_async_copy(ref, ref, sem).wait()

    barrier = pltpu.get_barrier_semaphore()
    for k in range(planes):
        for j in range(per):
            if k or j:
                pl.semaphore_signal(barrier, inc=1, device_id=device(k, j), device_id_type=MESH)

    load_first = pltpu.make_async_copy(first_hbm.at[0], first, weight_sem.at[0])
    load_second = pltpu.make_async_copy(second_hbm.at[0], second, weight_sem.at[1])
    load_first.start()
    load_second.start()

    def place_of(ids):
        offset = jnp.bitwise_xor(ids, me)
        return (offset % cols) // low, offset // cols + rows * (offset % low)

    def ones_at(condition):
        return jnp.where(condition, 1.0, 0.0).astype(jnp.bfloat16)

    ids_row = ids_row_ref[...]
    at_row = lax.broadcasted_iota(jnp.int32, (tok_rows, tok_rows), 0)
    at_col = lax.broadcasted_iota(jnp.int32, (tok_rows, tok_rows), 1)
    hot = lax.broadcasted_iota(jnp.int32, (lanes, tok_rows), 0) == ids_row
    hot_bf = ones_at(hot)
    earlier = jnp.dot(hot_bf, ones_at(at_row < at_col), preferred_element_type=jnp.float32)
    within = jnp.sum(jnp.where(hot, earlier, 0.0), axis=0, keepdims=True)
    plane_e, near_e = place_of(lax.broadcasted_iota(jnp.int32, (lanes, 1), 0))
    plane_t, near_t = place_of(ids_row)
    count_e = jnp.sum(jnp.where(hot, 1.0, 0.0), axis=1, keepdims=True)
    sooner = (plane_e == plane_t) & (near_e < near_t)
    ahead = jnp.sum(jnp.where(sooner, count_e, 0.0), axis=0, keepdims=True)
    start = jnp.where(plane_t == 0, near_t * cap, ahead.astype(jnp.int32))
    placed_row = plane_t * span + start + within.astype(jnp.int32)

    wide = tokens_ref[...].astype(jnp.float32)
    scale = lax.rsqrt(jnp.mean(wide * wide, axis=1, keepdims=True) + 1e-06)
    normed[...] = (wide * scale * gain_ref[...]).astype(jnp.bfloat16)

    tally = lax.dot_general(
        jnp.ones((8, tok_rows), jnp.bfloat16), hot_bf,
        (((1,), (1,)), ((), ())), preferred_element_type=jnp.float32,
    )[0:1]
    lane = lax.broadcasted_iota(jnp.int32, (1, lanes), 1)
    plane_l, _ = place_of(lane)
    over = jnp.zeros((1, 1), jnp.float32)
    for k in far:
        held = jnp.sum(jnp.where(plane_l == k, tally, 0.0), axis=1, keepdims=True)
        over = over + jnp.where(held > keep, 1.0, 0.0)
    counts[...] = tally + jnp.where(lane == n, over, 0.0)

    def columns(h):
        return pl.ds(h * wide_part, wide_part)

    def gather_from(k, size):
        slot = lax.broadcasted_iota(jnp.int32, (size, tok_rows), 0) + k * span
        return ones_at(slot == placed_row)

    def pack(k):
        table = gather_from(k, keep)
        for h in range(parts):
            packed[k, h] = jnp.dot(
                table, normed[:, columns(h)], preferred_element_type=jnp.float32
            ).astype(jnp.bfloat16)

    def send_far(k):
        for h in range(parts):
            send(packed.at[k, h], packed_in.at[k, h], send_sem.at[0], far_sem.at[k, h], device(k, 0))

    def send_near(source, target, out_sem, sem, k, h):
        for j in range(1, per):
            block = pl.ds(j * cap, cap)
            send(
                source.at[k, h, block], target.at[k, h, block], out_sem, sem.at[k, h], device(0, j)
            )

    def wait_near(target, sem, k, h, name):
        wait(target.at[k, h, pl.ds(cap, span - cap)], sem.at[k, h], f"{name}#k={k}#h={h}")

    def fill(k, h, values):
        made = values.astype(jnp.bfloat16)
        slots_in[k, h, 0:cap] = made[0:cap]
        slots[k, h] = made
        send_near(slots, slots_in, send_sem.at[1], near_sem, k, h)

    pack(far[0])
    with jax.named_scope("barrier_wait"):
        pl.semaphore_wait(barrier, n - 1)
    for k in far:
        send(counts, counts_far.at[k], send_sem.at[4], count_sem.at[0], device(k, 0))
    send_far(far[0])
    table = gather_from(0, span)
    for h in range(parts):
        fill(0, h, jnp.dot(table, normed[:, columns(h)], preferred_element_type=jnp.float32))
    for k in sent[1:]:
        pack(k)
        send_far(k)
    for k in range(planes):
        for j in range(1, per):
            send(
                counts, counts_in.at[k * (per - 1) + j - 1], send_sem.at[5], count_sem.at[1],
                device(k, j),
            )

    def to_column(row, size):
        there = lax.broadcasted_iota(jnp.int32, (size, size), 0)
        here = lax.broadcasted_iota(jnp.int32, (size, size), 1)
        return jnp.sum(jnp.where(there == here, row, 0.0), axis=1, keepdims=True)

    placed_col[...] = to_column(placed_row.astype(jnp.float32), tok_rows).astype(jnp.int32)
    gate_col[...] = to_column(gate_row_ref[...], tok_rows)

    wait(counts_far.at[pl.ds(1, planes - 1)], count_sem.at[0], "wait_counts")
    expert = lax.broadcasted_iota(jnp.int32, (lanes, span), 0)
    plane_s, near_s = place_of(expert)
    here = (plane_s == 0) & (expert < n)
    slot = lax.broadcasted_iota(jnp.int32, (lanes, span), 1)
    at_block = ones_at(here & (near_s == slot // cap))
    before_block = ones_at(here & (near_s < slot // cap))
    slot_row = lax.broadcasted_iota(jnp.int32, (1, span), 1)
    rank = (slot_row % cap).astype(jnp.float32)
    for k in far:
        tall = jnp.broadcast_to(counts_far[k], (8, lanes)).astype(jnp.bfloat16)
        held = jnp.dot(tall, at_block, preferred_element_type=jnp.float32)[0:1]
        begin = jnp.dot(tall, before_block, preferred_element_type=jnp.float32)[0:1]
        index = jnp.where(rank < held, begin + rank, -1.0)
        index_row[k] = index.astype(jnp.int32)
        index_col[k] = to_column(index, span).astype(jnp.int32)

    with jax.named_scope("wait_weights"):
        load_first.wait()
        load_second.wait()

    def relay(k, h):
        wait(packed_in.at[k, h], far_sem.at[k, h], f"wait_far#k={k}#h={h}")
        slot = lax.broadcasted_iota(jnp.int32, (span, keep), 1)
        table = ones_at(slot == index_col[k])
        fill(k, h, jnp.dot(table, packed_in[k, h], preferred_element_type=jnp.float32))

    def grow(k):
        for h in range(parts):
            wait_near(slots_in, near_sem, k, h, "wait_slots")

        @pl.loop(0, first.shape[1] // ff_tile)
        def _(i):
            part = pl.ds(pl.multiple_of(i * ff_tile, ff_tile), ff_tile)
            grown = jnp.dot(slots_in[k, 0], first[columns(0), part], preferred_element_type=jnp.float32)
            for h in range(1, parts):
                grown += jnp.dot(
                    slots_in[k, h], first[columns(h), part], preferred_element_type=jnp.float32
                )
            hidden[:, part] = jnp.maximum(grown, 0.0).astype(jnp.bfloat16)

    def shrink(k, h):
        @pl.loop(0, wide_part // out_tile)
        def _(i):
            at = pl.multiple_of(i * out_tile, out_tile)
            part = pl.ds(pl.multiple_of(h * wide_part + i * out_tile, out_tile), out_tile)
            made = jnp.dot(hidden[...], second[:, part], preferred_element_type=jnp.float32)
            made = made.astype(jnp.bfloat16)
            answers[k, h, :, pl.ds(at, out_tile)] = made
            answers_in[k, h, 0:cap, pl.ds(at, out_tile)] = made[0:cap]

    def send_answers(k, h):
        send_near(answers, answers_in, send_sem.at[2], answer_sem, k, h)

    def give_back(k, h):
        wait_near(answers_in, answer_sem, k, h, "wait_answers")
        slot = lax.broadcasted_iota(jnp.int32, (keep, span), 0)
        table = ones_at(slot == index_row[k])
        back[k, h] = jnp.dot(
            table, answers_in[k, h], preferred_element_type=jnp.float32
        ).astype(jnp.bfloat16)
        send(back.at[k, h], back_in.at[k, h], send_sem.at[3], back_sem.at[k, h], device(k, 0))

    def picked(k, h):
        size = keep if k else span
        if k:
            wait(back_in.at[k, h], back_sem.at[k, h], f"wait_back#k={k}#h={h}")
        else:
            wait_near(answers_in, answer_sem, 0, h, "wait_answers")
        source = back_in if k else answers_in
        slot = lax.broadcasted_iota(jnp.int32, (tok_rows, size), 1) + k * span
        table = ones_at(slot == placed_col[...])
        return jnp.dot(table, source[k, h], preferred_element_type=jnp.float32)

    halves = range(parts)
    grow(0)
    for h in halves:
        shrink(0, h)
    for h in halves:
        relay(far[0], h)
    todo = far[:1] + far[:0:-1]
    for i, k in enumerate(todo):
        grow(k)
        after = todo[i + 1] if i + 1 < len(todo) else None
        last = i + 2 == len(todo)
        if after is not None:
            relay(after, 0)
            if last:
                give_back(todo[i - 1], 0)
                for h in range(1, parts):
                    give_back(todo[i - 1], h)
            for h in range(1, parts):
                relay(after, h)
        for h in halves:
            if after is None and i:
                give_back(todo[i - 1], h)
            shrink(k, h)
            send_answers(k, h)
    for h in halves:
        send_answers(0, h)
    for h in halves:
        give_back(todo[-1], h)

    wait(counts_in, count_sem.at[1])
    sums = jnp.sum(counts_in[...], axis=0) + counts[...]
    sums += jnp.sum(counts_far[pl.ds(1, planes - 1)], axis=0)
    routed_ref[0] = jnp.sum(jnp.where(lane == me, sums, 0.0)).astype(jnp.int32)
    over_ref[0] = jnp.sum(jnp.where(lane == n, sums, 0.0)).astype(jnp.int32)

    for h in range(parts):
        total[h] = picked(0, h)
    for k in todo[:-1]:
        for h in range(parts):
            total[h] += picked(k, h)
    for h in range(parts):
        found = total[h] + picked(todo[-1], h)
        kept = tokens_ref[:, columns(h)].astype(jnp.float32)
        mixed_ref[:, columns(h)] = (kept + gate_col[...] * found).astype(jnp.bfloat16)

    wait(packed.at[pl.ds(1, planes - 1)], send_sem.at[0])
    wait(slots.at[:, :, pl.ds(cap, span - cap)], send_sem.at[1])
    wait(answers.at[:, :, pl.ds(cap, span - cap)], send_sem.at[2])
    wait(back.at[pl.ds(1, planes - 1)], send_sem.at[3])
    wait(counts_far.at[pl.ds(1, planes - 1)], send_sem.at[4])
    wait(counts_in, send_sem.at[5])


def packed_layer(rows, cols, tokens, expert_ids, gate_prob, norm_gain, weight_in, weight_out):
    tok_rows, width = tokens.shape
    hidden_width = weight_in.shape[2]
    n = rows * cols
    low = min(2, cols)
    planes = cols // low
    per = n // planes
    cap = 2 * tok_rows // n
    span = per * cap
    keep = 3 * span // 4
    parts = 2
    part = width // parts
    lanes = -(-(n + 1) // 128) * 128
    vmem = pl.BlockSpec(memory_space=pltpu.VMEM)
    smem = pl.BlockSpec(memory_space=pltpu.SMEM)
    hbm = pl.BlockSpec(memory_space=pl.ANY)
    tight = pltpu.VMEM((planes, parts, keep, part), jnp.bfloat16)
    loose = pltpu.VMEM((planes, parts, span, part), jnp.bfloat16)
    each = pltpu.SemaphoreType.DMA((planes, parts))
    return pl.pallas_call(
        functools.partial(
            packed_kernel, rows, cols, low, cap, keep, parts,
            min(512, hidden_width), min(256, part),
        ),
        out_shape=(
            jax.ShapeDtypeStruct((tok_rows, width), jnp.bfloat16),
            jax.ShapeDtypeStruct((1,), jnp.int32),
            jax.ShapeDtypeStruct((1,), jnp.int32),
        ),
        in_specs=[vmem, vmem, vmem, vmem, hbm, hbm],
        out_specs=(vmem, smem, smem),
        scratch_shapes=[
            pltpu.VMEM((width, hidden_width), jnp.bfloat16),
            pltpu.VMEM((hidden_width, width), jnp.bfloat16),
            pltpu.VMEM((tok_rows, width), jnp.bfloat16),
            tight, tight, loose, loose, loose, loose, tight, tight,
            pltpu.VMEM((span, hidden_width), jnp.bfloat16),
            pltpu.VMEM((parts, tok_rows, part), jnp.float32),
            pltpu.VMEM((1, lanes), jnp.float32),
            pltpu.VMEM((planes, 1, lanes), jnp.float32),
            pltpu.VMEM((planes * (per - 1), 1, lanes), jnp.float32),
            pltpu.VMEM((planes, 1, span), jnp.int32),
            pltpu.VMEM((planes, span, 1), jnp.int32),
            pltpu.VMEM((tok_rows, 1), jnp.int32),
            pltpu.VMEM((tok_rows, 1), jnp.float32),
            pltpu.SemaphoreType.DMA((2,)),
            pltpu.SemaphoreType.DMA((6,)),
            each, each, each, each,
            pltpu.SemaphoreType.DMA((2,)),
        ],
        compiler_params=pltpu.CompilerParams(
            collective_id=0, has_side_effects=True, vmem_limit_bytes=56 * 1024 * 1024
        ),
    )(
        tokens,
        expert_ids.reshape(1, tok_rows),
        gate_prob.reshape(1, tok_rows),
        norm_gain.reshape(1, width),
        weight_in,
        weight_out,
    )


def slotted_layer(rows, cols, tokens, expert_ids, gate_prob, norm_gain, weight_in, weight_out):
    tok_rows, width = tokens.shape
    hidden_width = weight_in.shape[2]
    n = rows * cols
    cap = 2 * tok_rows // n
    lanes = -(-n // 128) * 128
    per = max(1, min(n, 256 // cap))
    groups = n // per
    vmem = pl.BlockSpec(memory_space=pltpu.VMEM)
    hbm = pl.BlockSpec(memory_space=pl.ANY)
    block = pltpu.VMEM((n, cap, width), jnp.bfloat16)
    back, routed = pl.pallas_call(
        functools.partial(kernel, rows, cols, cap, groups, min(512, hidden_width), min(256, width)),
        out_shape=(
            jax.ShapeDtypeStruct((tok_rows, width), jnp.bfloat16),
            jax.ShapeDtypeStruct((1,), jnp.int32),
        ),
        in_specs=[vmem, vmem, vmem, hbm, hbm],
        out_specs=(vmem, pl.BlockSpec(memory_space=pltpu.SMEM)),
        scratch_shapes=[
            pltpu.VMEM((width, hidden_width), jnp.bfloat16),
            pltpu.VMEM((hidden_width, width), jnp.bfloat16),
            pltpu.VMEM((tok_rows, width), jnp.bfloat16),
            block, block, block, block,
            pltpu.VMEM((per * cap, hidden_width), jnp.bfloat16),
            pltpu.VMEM((tok_rows, width), jnp.float32),
            pltpu.VMEM((1, lanes), jnp.float32),
            pltpu.VMEM((n, 1, lanes), jnp.float32),
            pltpu.VMEM((tok_rows, 1), jnp.int32),
            pltpu.SemaphoreType.DMA((2,)),
            pltpu.SemaphoreType.DMA((3,)),
            pltpu.SemaphoreType.DMA((groups,)),
            pltpu.SemaphoreType.DMA((groups,)),
            pltpu.SemaphoreType.DMA,
        ],
        compiler_params=pltpu.CompilerParams(
            collective_id=1, has_side_effects=True, vmem_limit_bytes=56 * 1024 * 1024
        ),
    )(
        tokens,
        expert_ids.reshape(1, tok_rows),
        norm_gain.reshape(1, width),
        weight_in,
        weight_out,
    )
    wide = tokens.astype(jnp.float32)
    mixed = (wide + gate_prob[:, None] * back.astype(jnp.float32)).astype(jnp.bfloat16)
    return mixed


def on_device(rows, cols, *args):
    mixed, routed, over = packed_layer(rows, cols, *args)
    mixed = lax.cond(
        over[0] > 0, lambda given, *all_args: slotted_layer(rows, cols, *all_args),
        lambda given, *all_args: given, mixed, *args,
    )
    return (mixed, routed)


def solution(mesh):
    return jax.shard_map(
        functools.partial(on_device, mesh.shape["row"], mesh.shape["col"]),
        mesh=mesh,
        in_specs=(
            P(("row", "col"), None),
            P(("row", "col"), None),
            P(("row", "col")),
            P(),
            P(("row", "col"), None, None),
            P(("row", "col"), None, None),
        ),
        out_specs=(P(("row", "col"), None), P(("row", "col"))),
        check_vma=False,
    )
```

```python
import functools

import jax
import jax.numpy as jnp
from jax import lax
from jax.experimental import pallas as pl
from jax.experimental.pallas import tpu as pltpu
from jax.sharding import PartitionSpec as P

MESH = pl.DeviceIdType.MESH


def bit_xor(a, b, size):
    out, unit = 0, 1
    while unit < size:
        out = out + lax.rem(lax.div(a, unit) + lax.div(b, unit), 2) * unit
        unit *= 2
    return out


def kernel(
    rows, cols, cap, groups, ff_tile, out_tile,
    tokens_ref, ids_row_ref, gain_ref, first_hbm, second_hbm,
    back_ref, routed_ref,
    first, second, normed, outgoing, received, answers, returned, hidden, total,
    counts, counts_in, placed_col,
    weight_sem, send_sem, recv_sem, ret_sem, count_sem,
):
    n = rows * cols
    tok_rows, width = tokens_ref.shape
    lanes = counts.shape[1]
    per = n // groups
    span = per * cap
    my_row, my_col = lax.axis_index("row"), lax.axis_index("col")
    me = my_row * cols + my_col

    def turn(step):
        if groups % 2:
            return step
        return lax.rem(step, 2) * (groups // 2) + lax.div(step, 2)

    def partner(place):
        q = n - 1 - place
        return (
            bit_xor(my_row, lax.rem(q, rows), rows),
            bit_xor(my_col, lax.div(q, rows), cols),
        )

    barrier = pltpu.get_barrier_semaphore()

    @pl.loop(0, n - 1)
    def _(place):
        pl.semaphore_signal(barrier, inc=1, device_id=partner(place), device_id_type=MESH)

    load_first = pltpu.make_async_copy(first_hbm.at[0], first, weight_sem.at[0])
    load_second = pltpu.make_async_copy(second_hbm.at[0], second, weight_sem.at[1])
    load_first.start()
    load_second.start()

    def slot_of(ids, within):
        offset = jnp.bitwise_xor(ids, me)
        q = (offset % cols) * rows + offset // cols
        return (n - 1 - q) * cap + within

    ids_row = ids_row_ref[...]
    at_row = lax.broadcasted_iota(jnp.int32, (tok_rows, tok_rows), 0)
    at_col = lax.broadcasted_iota(jnp.int32, (tok_rows, tok_rows), 1)
    hot_row = lax.broadcasted_iota(jnp.int32, (lanes, tok_rows), 0) == ids_row
    before = jnp.where(at_row < at_col, 1.0, 0.0).astype(jnp.bfloat16)
    earlier = jnp.dot(
        jnp.where(hot_row, 1.0, 0.0).astype(jnp.bfloat16), before, preferred_element_type=jnp.float32
    )
    within_row = jnp.sum(jnp.where(hot_row, earlier, 0.0), axis=0, keepdims=True)
    placed_row = slot_of(ids_row, within_row.astype(jnp.int32))

    wide = tokens_ref[...].astype(jnp.float32)
    scale = lax.rsqrt(jnp.mean(wide * wide, axis=1, keepdims=True) + 1e-06)
    normed[...] = (wide * scale * gain_ref[...]).astype(jnp.bfloat16)

    def as_blocks(values):
        return values.reshape(per, cap, width).astype(jnp.bfloat16)

    def as_rows(ref, g):
        blocks = ref[pl.ds(g * per, per)]
        if cap % 16 == 0:
            return blocks.reshape(span, width)
        return blocks.astype(jnp.float32).reshape(span, width).astype(jnp.bfloat16)

    def exchange(source, target, sem, out_sem, g):
        @pl.loop(0, per)
        def _(i):
            place = g * per + i

            @pl.when(place < n - 1)
            def _():
                pltpu.make_async_remote_copy(
                    src_ref=source.at[place],
                    dst_ref=target.at[place],
                    send_sem=out_sem,
                    recv_sem=sem.at[g],
                    device_id=partner(place),
                    device_id_type=MESH,
                ).start()

            @pl.when(place == n - 1)
            def _():
                pltpu.make_async_copy(source.at[n - 1], target.at[n - 1], sem.at[g]).start()

    def wait_group(target, sem, g):
        whole = target.at[pl.ds(g * per, per)]
        pltpu.make_async_copy(whole, whole, sem.at[g]).wait()

    @pl.loop(0, groups)
    def _(step):
        g = turn(step)
        slot = lax.broadcasted_iota(jnp.int32, (span, tok_rows), 0) + g * span
        table = jnp.where(slot == placed_row, 1.0, 0.0).astype(jnp.bfloat16)
        outgoing[pl.ds(g * per, per)] = as_blocks(
            jnp.dot(table, normed[...], preferred_element_type=jnp.float32)
        )

        @pl.when(step == 0)
        def _():
            pl.semaphore_wait(barrier, n - 1)

        exchange(outgoing, received, recv_sem, send_sem.at[0], g)

    counts[...] = lax.dot_general(
        jnp.ones((8, tok_rows), jnp.bfloat16),
        jnp.where(hot_row, 1.0, 0.0).astype(jnp.bfloat16),
        (((1,), (1,)), ((), ())),
        preferred_element_type=jnp.float32,
    )[0:1]
    turned = jnp.where(at_row == at_col, placed_row.astype(jnp.float32), 0.0)
    placed_col[...] = jnp.sum(turned, axis=1, keepdims=True).astype(jnp.int32)
    total[...] = jnp.zeros_like(total)

    @pl.loop(0, n - 1)
    def _(place):
        pltpu.make_async_remote_copy(
            src_ref=counts,
            dst_ref=counts_in.at[place],
            send_sem=send_sem.at[2],
            recv_sem=count_sem,
            device_id=partner(place),
            device_id_type=MESH,
        ).start()

    load_first.wait()
    load_second.wait()

    @pl.loop(0, groups)
    def _(step):
        g = turn(lax.rem(step + groups - 1, groups))
        wait_group(received, recv_sem, g)
        slab = as_rows(received, g)

        @pl.loop(0, first.shape[1] // ff_tile)
        def _(i):
            part = pl.ds(pl.multiple_of(i * ff_tile, ff_tile), ff_tile)
            grown = jnp.dot(slab, first[:, part], preferred_element_type=jnp.float32)
            hidden[:, part] = jnp.maximum(grown, 0.0).astype(jnp.bfloat16)

        @pl.loop(0, width // out_tile)
        def _(i):
            part = pl.ds(pl.multiple_of(i * out_tile, out_tile), out_tile)
            made = jnp.dot(hidden[...], second[:, part], preferred_element_type=jnp.float32)
            answers[pl.ds(g * per, per), :, part] = made.reshape(per, cap, out_tile).astype(
                jnp.bfloat16
            )

        exchange(answers, returned, ret_sem, send_sem.at[1], g)

    arrived = counts_in.at[pl.ds(0, n - 1)]
    pltpu.make_async_copy(arrived, arrived, count_sem).wait()
    sums = jnp.sum(counts_in[pl.ds(0, n - 1)], axis=0) + counts[...]
    mine = lax.broadcasted_iota(jnp.int32, (1, lanes), 1) == me
    routed_ref[0] = jnp.sum(jnp.where(mine, sums, 0.0)).astype(jnp.int32)

    @pl.loop(0, groups)
    def _(step):
        g = turn(lax.rem(step + groups - 1, groups))
        wait_group(returned, ret_sem, g)
        slot = lax.broadcasted_iota(jnp.int32, (tok_rows, span), 1) + g * span
        table = jnp.where(slot == placed_col[...], 1.0, 0.0).astype(jnp.bfloat16)
        total[...] += jnp.dot(table, as_rows(returned, g), preferred_element_type=jnp.float32)

    back_ref[...] = total[...].astype(jnp.bfloat16)

    sent = outgoing.at[pl.ds(0, n - 1)]
    pltpu.make_async_copy(sent, sent, send_sem.at[0]).wait()
    pltpu.make_async_copy(sent, sent, send_sem.at[1]).wait()
    pltpu.make_async_copy(arrived, arrived, send_sem.at[2]).wait()


def flipped(a, mask, size):
    out, unit = 0, 1
    while unit < size:
        bit = lax.rem(lax.div(a, unit), 2)
        out = out + ((1 - bit) if (mask // unit) % 2 else bit) * unit
        unit *= 2
    return out


def packed_kernel(
    rows, cols, low, cap, keep, parts, ff_tile, out_tile,
    tokens_hbm, ids_hbm, gate_hbm, gain_hbm, first_hbm, second_hbm,
    mixed_hbm, routed_ref, over_ref,
    tokens_ref, ids_row_ref, gate_row_ref, gain_ref, mixed_ref, first, second, normed, packed, packed_in, slots, slots_in, answers, answers_in,
    back, back_in, hidden, total, counts, counts_far, sums, sums_in,
    index_row, index_col, placed_col, gate_col,
    load_sem, store_sem, send_sem, far_sem, near_sem, answer_sem, back_sem, count_sem,
):
    n = rows * cols
    planes = cols // low
    per = n // planes
    span = per * cap
    tok_rows, width = tokens_ref.shape
    wide_part = width // parts
    lanes = counts.shape[1]
    my_row, my_col = lax.axis_index("row"), lax.axis_index("col")
    me = my_row * cols + my_col
    row_at = [flipped(my_row, c, rows) for c in range(rows)]
    low_at = [flipped(lax.rem(my_col, low), c, low) for c in range(low)]
    plane_at = [flipped(lax.div(my_col, low), c, planes) * low for c in range(planes)]
    far = list(range(planes - 1, 0, -1))
    half = planes // 2
    sent = [planes - 1 - k for i in range(half) for k in (i, i + half)][: planes - 1]
    if planes % 2:
        sent = far

    def device(k, j):
        return (row_at[j % rows], plane_at[k] + low_at[j // rows])

    def send(source, target, out_sem, sem, where):
        pltpu.make_async_remote_copy(
            src_ref=source, dst_ref=target, send_sem=out_sem, recv_sem=sem,
            device_id=where, device_id_type=MESH,
        ).start()

    def wait(ref, sem, name="wait_last"):
        with jax.named_scope(name):
            pltpu.make_async_copy(ref, ref, sem).wait()

    barrier = pltpu.get_barrier_semaphore()
    near_by = [(0, j) for j in range(1, per)]
    peers = [(k, 0) for k in far] + near_by
    for k, j in peers:
        pl.semaphore_signal(barrier, inc=1, device_id=device(k, j), device_id_type=MESH)

    loads = [
        pltpu.make_async_copy(source, target, load_sem.at[i])
        for i, (source, target) in enumerate(
            (
                (ids_hbm, ids_row_ref), (tokens_hbm, tokens_ref), (gain_hbm, gain_ref),
                (gate_hbm, gate_row_ref), (first_hbm.at[0], first), (second_hbm.at[0], second),
            )
        )
    ]
    for load in loads:
        load.start()
    loads[0].wait()

    def place_of(ids):
        offset = jnp.bitwise_xor(ids, me)
        return (offset % cols) // low, offset // cols + rows * (offset % low)

    def ones_at(condition):
        return jnp.where(condition, 1.0, 0.0).astype(jnp.bfloat16)

    ids_row = ids_row_ref[...]
    at_row = lax.broadcasted_iota(jnp.int32, (tok_rows, tok_rows), 0)
    at_col = lax.broadcasted_iota(jnp.int32, (tok_rows, tok_rows), 1)
    hot = lax.broadcasted_iota(jnp.int32, (lanes, tok_rows), 0) == ids_row
    hot_bf = ones_at(hot)
    earlier = jnp.dot(hot_bf, ones_at(at_row < at_col), preferred_element_type=jnp.float32)
    within = jnp.sum(jnp.where(hot, earlier, 0.0), axis=0, keepdims=True)
    plane_e, near_e = place_of(lax.broadcasted_iota(jnp.int32, (lanes, 1), 0))
    plane_t, near_t = place_of(ids_row)
    count_e = jnp.sum(jnp.where(hot, 1.0, 0.0), axis=1, keepdims=True)
    sooner = (plane_e == plane_t) & (near_e < near_t)
    ahead = jnp.sum(jnp.where(sooner, count_e, 0.0), axis=0, keepdims=True)
    start = jnp.where(plane_t == 0, near_t * cap, ahead.astype(jnp.int32))
    placed_row = plane_t * span + start + within.astype(jnp.int32)

    loads[1].wait()
    loads[2].wait()
    wide = tokens_ref[...].astype(jnp.float32)
    scale = lax.rsqrt(jnp.mean(wide * wide, axis=1, keepdims=True) + 1e-06)
    normed[...] = (wide * scale * gain_ref[...]).astype(jnp.bfloat16)

    tally = lax.dot_general(
        jnp.ones((8, tok_rows), jnp.bfloat16), hot_bf,
        (((1,), (1,)), ((), ())), preferred_element_type=jnp.float32,
    )[0:1]
    lane = lax.broadcasted_iota(jnp.int32, (1, lanes), 1)
    plane_l, _ = place_of(lane)
    over = jnp.zeros((1, 1), jnp.float32)
    for k in far:
        held = jnp.sum(jnp.where(plane_l == k, tally, 0.0), axis=1, keepdims=True)
        over = over + jnp.where(held > keep, 1.0, 0.0)
    counts[...] = tally + jnp.where(lane == n, over, 0.0)

    def columns(h):
        return pl.ds(h * wide_part, wide_part)

    def gather_from(k, size):
        slot = lax.broadcasted_iota(jnp.int32, (size, tok_rows), 0) + k * span
        return ones_at(slot == placed_row)

    def pack(k):
        table = gather_from(k, keep)
        for h in range(parts):
            packed[k, h] = jnp.dot(
                table, normed[:, columns(h)], preferred_element_type=jnp.float32
            ).astype(jnp.bfloat16)

    def send_far(k):
        for h in range(parts):
            send(packed.at[k, h], packed_in.at[k, h], send_sem.at[0], far_sem.at[k, h], device(k, 0))

    def send_near(source, target, out_sem, sem, k, h):
        for j in range(1, per):
            block = pl.ds(j * cap, cap)
            send(
                source.at[k, h, block], target.at[k, h, block], out_sem, sem.at[k, h], device(0, j)
            )

    def wait_near(target, sem, k, h, name):
        wait(target.at[k, h, pl.ds(cap, span - cap)], sem.at[k, h], f"{name}#k={k}#h={h}")

    def fill(k, h, values):
        made = values.astype(jnp.bfloat16)
        slots_in[k, h, 0:cap] = made[0:cap]
        slots[k, h] = made
        send_near(slots, slots_in, send_sem.at[1], near_sem, k, h)

    pack(far[0])
    with jax.named_scope("barrier_wait"):
        pl.semaphore_wait(barrier, len(peers))
    for k in far:
        send(counts, counts_far.at[k], send_sem.at[4], count_sem.at[0], device(k, 0))
    send_far(far[0])
    table = gather_from(0, span)
    for h in range(parts):
        fill(0, h, jnp.dot(table, normed[:, columns(h)], preferred_element_type=jnp.float32))
    for k in sent[1:]:
        pack(k)
        send_far(k)
    def to_column(row, size):
        there = lax.broadcasted_iota(jnp.int32, (size, size), 0)
        here = lax.broadcasted_iota(jnp.int32, (size, size), 1)
        return jnp.sum(jnp.where(there == here, row, 0.0), axis=1, keepdims=True)

    placed_col[...] = to_column(placed_row.astype(jnp.float32), tok_rows).astype(jnp.int32)
    loads[3].wait()
    gate_col[...] = to_column(gate_row_ref[...], tok_rows)

    wait(counts_far.at[pl.ds(1, planes - 1)], count_sem.at[0], "wait_counts")
    sums[...] = counts[...] + jnp.sum(counts_far[pl.ds(1, planes - 1)], axis=0)
    for k, j in near_by:
        send(sums, sums_in.at[j], send_sem.at[5], count_sem.at[1], device(k, j))
    expert = lax.broadcasted_iota(jnp.int32, (lanes, span), 0)
    plane_s, near_s = place_of(expert)
    here = (plane_s == 0) & (expert < n)
    slot = lax.broadcasted_iota(jnp.int32, (lanes, span), 1)
    at_block = ones_at(here & (near_s == slot // cap))
    before_block = ones_at(here & (near_s < slot // cap))
    slot_row = lax.broadcasted_iota(jnp.int32, (1, span), 1)
    rank = (slot_row % cap).astype(jnp.float32)
    for k in far:
        tall = jnp.broadcast_to(counts_far[k], (8, lanes)).astype(jnp.bfloat16)
        held = jnp.dot(tall, at_block, preferred_element_type=jnp.float32)[0:1]
        begin = jnp.dot(tall, before_block, preferred_element_type=jnp.float32)[0:1]
        index = jnp.where(rank < held, begin + rank, -1.0)
        index_row[k] = index.astype(jnp.int32)
        index_col[k] = to_column(index, span).astype(jnp.int32)

    with jax.named_scope("wait_weights"):
        loads[4].wait()
        loads[5].wait()

    def relay(k, h):
        wait(packed_in.at[k, h], far_sem.at[k, h], f"wait_far#k={k}#h={h}")
        slot = lax.broadcasted_iota(jnp.int32, (span, keep), 1)
        table = ones_at(slot == index_col[k])
        fill(k, h, jnp.dot(table, packed_in[k, h], preferred_element_type=jnp.float32))

    def await_slots(k):
        for h in range(parts):
            wait_near(slots_in, near_sem, k, h, "wait_slots")

    def grow(k):
        @pl.loop(0, first.shape[1] // ff_tile, unroll=min(4, first.shape[1] // ff_tile))
        def _(i):
            part = pl.ds(pl.multiple_of(i * ff_tile, ff_tile), ff_tile)
            grown = jnp.dot(slots_in[k, 0], first[columns(0), part], preferred_element_type=jnp.float32)
            for h in range(1, parts):
                grown += jnp.dot(
                    slots_in[k, h], first[columns(h), part], preferred_element_type=jnp.float32
                )
            hidden[:, part] = jnp.maximum(grown, 0.0).astype(jnp.bfloat16)

    def shrink(k, h):
        @pl.loop(0, wide_part // out_tile, unroll=True)
        def _(i):
            at = pl.multiple_of(i * out_tile, out_tile)
            part = pl.ds(pl.multiple_of(h * wide_part + i * out_tile, out_tile), out_tile)
            made = jnp.dot(hidden[...], second[:, part], preferred_element_type=jnp.float32)
            made = made.astype(jnp.bfloat16)
            answers[k, h, :, pl.ds(at, out_tile)] = made
            answers_in[k, h, 0:cap, pl.ds(at, out_tile)] = made[0:cap]

    def send_answers(k, h):
        send_near(answers, answers_in, send_sem.at[2], answer_sem, k, h)

    def give_back(k, h):
        wait_near(answers_in, answer_sem, k, h, "wait_answers")
        slot = lax.broadcasted_iota(jnp.int32, (keep, span), 0)
        table = ones_at(slot == index_row[k])
        back[k, h] = jnp.dot(
            table, answers_in[k, h], preferred_element_type=jnp.float32
        ).astype(jnp.bfloat16)
        send(back.at[k, h], back_in.at[k, h], send_sem.at[3], back_sem.at[k, h], device(k, 0))

    def picked(k, h):
        size = keep if k else span
        if k:
            wait(back_in.at[k, h], back_sem.at[k, h], f"wait_back#k={k}#h={h}")
        else:
            wait_near(answers_in, answer_sem, 0, h, "wait_answers")
        source = back_in if k else answers_in
        slot = lax.broadcasted_iota(jnp.int32, (tok_rows, size), 1) + k * span
        table = ones_at(slot == placed_col[...])
        return jnp.dot(table, source[k, h], preferred_element_type=jnp.float32)

    halves = range(parts)
    todo = far[:1] + far[:0:-1]
    await_slots(0)
    grow(0)
    for h in halves:
        shrink(0, h)
    for k in todo[:2]:
        for h in halves:
            relay(k, h)
    for i, k in enumerate(todo):
        await_slots(k)
        grow(k)
        behind = todo[i + 1 : i + 2] if i else []
        for k2 in behind:
            relay(k2, 0)
        for h in halves:
            if i == 1:
                give_back(todo[0], h)
        for k2 in behind:
            for h in range(1, parts):
                relay(k2, h)
        for h in halves:
            shrink(k, h)
            send_answers(k, h)
            if i > 1:
                give_back(todo[i - 1], h)
    for h in halves:
        give_back(todo[-1], h)
    for h in halves:
        send_answers(0, h)

    wait(sums_in.at[pl.ds(1, per - 1)], count_sem.at[1])
    whole = sums[...] + jnp.sum(sums_in[pl.ds(1, per - 1)], axis=0)
    routed_ref[0] = jnp.sum(jnp.where(lane == me, whole, 0.0)).astype(jnp.int32)
    over_ref[0] = jnp.sum(jnp.where(lane == n, whole, 0.0)).astype(jnp.int32)

    for h in range(parts):
        total[h] = picked(0, h)
    for k in todo[:-1]:
        for h in range(parts):
            total[h] += picked(k, h)
    for h in range(parts):
        found = total[h] + picked(todo[-1], h)
        kept = tokens_ref[:, columns(h)].astype(jnp.float32)
        mixed_ref[:, columns(h)] = (kept + gate_col[...] * found).astype(jnp.bfloat16)
        pltpu.make_async_copy(
            mixed_ref.at[:, columns(h)], mixed_hbm.at[:, columns(h)], store_sem.at[h]
        ).start()

    wait(packed.at[pl.ds(1, planes - 1)], send_sem.at[0])
    wait(slots.at[:, :, pl.ds(cap, span - cap)], send_sem.at[1])
    wait(answers.at[:, :, pl.ds(cap, span - cap)], send_sem.at[2])
    wait(back.at[pl.ds(1, planes - 1)], send_sem.at[3])
    wait(counts_far.at[pl.ds(1, planes - 1)], send_sem.at[4])
    wait(sums_in.at[pl.ds(1, per - 1)], send_sem.at[5])
    for h in halves:
        wait(mixed_ref.at[:, columns(h)], store_sem.at[h])


def packed_layer(rows, cols, tokens, expert_ids, gate_prob, norm_gain, weight_in, weight_out):
    tok_rows, width = tokens.shape
    hidden_width = weight_in.shape[2]
    n = rows * cols
    low = min(2, cols)
    planes = cols // low
    per = n // planes
    cap = 2 * tok_rows // n
    span = per * cap
    keep = 3 * span // 4
    parts = 2
    part = width // parts
    lanes = -(-(n + 1) // 128) * 128
    smem = pl.BlockSpec(memory_space=pltpu.SMEM)
    hbm = pl.BlockSpec(memory_space=pl.ANY)
    tight = pltpu.VMEM((planes, parts, keep, part), jnp.bfloat16)
    loose = pltpu.VMEM((planes, parts, span, part), jnp.bfloat16)
    each = pltpu.SemaphoreType.DMA((planes, parts))
    return pl.pallas_call(
        functools.partial(
            packed_kernel, rows, cols, low, cap, keep, parts,
            min(512, hidden_width), min(256, part),
        ),
        out_shape=(
            jax.ShapeDtypeStruct((tok_rows, width), jnp.bfloat16),
            jax.ShapeDtypeStruct((1,), jnp.int32),
            jax.ShapeDtypeStruct((1,), jnp.int32),
        ),
        in_specs=[hbm, hbm, hbm, hbm, hbm, hbm],
        out_specs=(hbm, smem, smem),
        scratch_shapes=[
            pltpu.VMEM((tok_rows, width), jnp.bfloat16),
            pltpu.VMEM((1, tok_rows), jnp.int32),
            pltpu.VMEM((1, tok_rows), jnp.float32),
            pltpu.VMEM((1, width), jnp.float32),
            pltpu.VMEM((tok_rows, width), jnp.bfloat16),
            pltpu.VMEM((width, hidden_width), jnp.bfloat16),
            pltpu.VMEM((hidden_width, width), jnp.bfloat16),
            pltpu.VMEM((tok_rows, width), jnp.bfloat16),
            tight, tight, loose, loose, loose, loose, tight, tight,
            pltpu.VMEM((span, hidden_width), jnp.bfloat16),
            pltpu.VMEM((parts, tok_rows, part), jnp.float32),
            pltpu.VMEM((1, lanes), jnp.float32),
            pltpu.VMEM((planes, 1, lanes), jnp.float32),
            pltpu.VMEM((1, lanes), jnp.float32),
            pltpu.VMEM((per, 1, lanes), jnp.float32),
            pltpu.VMEM((planes, 1, span), jnp.int32),
            pltpu.VMEM((planes, span, 1), jnp.int32),
            pltpu.VMEM((tok_rows, 1), jnp.int32),
            pltpu.VMEM((tok_rows, 1), jnp.float32),
            pltpu.SemaphoreType.DMA((6,)),
            pltpu.SemaphoreType.DMA((parts,)),
            pltpu.SemaphoreType.DMA((6,)),
            each, each, each, each,
            pltpu.SemaphoreType.DMA((2,)),
        ],
        compiler_params=pltpu.CompilerParams(
            collective_id=0, has_side_effects=True, vmem_limit_bytes=56 * 1024 * 1024
        ),
    )(
        tokens,
        expert_ids.reshape(1, tok_rows),
        gate_prob.reshape(1, tok_rows),
        norm_gain.reshape(1, width),
        weight_in,
        weight_out,
    )


def slotted_layer(rows, cols, tokens, expert_ids, gate_prob, norm_gain, weight_in, weight_out):
    tok_rows, width = tokens.shape
    hidden_width = weight_in.shape[2]
    n = rows * cols
    cap = 2 * tok_rows // n
    lanes = -(-n // 128) * 128
    per = max(1, min(n, 256 // cap))
    groups = n // per
    vmem = pl.BlockSpec(memory_space=pltpu.VMEM)
    hbm = pl.BlockSpec(memory_space=pl.ANY)
    block = pltpu.VMEM((n, cap, width), jnp.bfloat16)
    back, routed = pl.pallas_call(
        functools.partial(kernel, rows, cols, cap, groups, min(512, hidden_width), min(256, width)),
        out_shape=(
            jax.ShapeDtypeStruct((tok_rows, width), jnp.bfloat16),
            jax.ShapeDtypeStruct((1,), jnp.int32),
        ),
        in_specs=[vmem, vmem, vmem, hbm, hbm],
        out_specs=(vmem, pl.BlockSpec(memory_space=pltpu.SMEM)),
        scratch_shapes=[
            pltpu.VMEM((width, hidden_width), jnp.bfloat16),
            pltpu.VMEM((hidden_width, width), jnp.bfloat16),
            pltpu.VMEM((tok_rows, width), jnp.bfloat16),
            block, block, block, block,
            pltpu.VMEM((per * cap, hidden_width), jnp.bfloat16),
            pltpu.VMEM((tok_rows, width), jnp.float32),
            pltpu.VMEM((1, lanes), jnp.float32),
            pltpu.VMEM((n, 1, lanes), jnp.float32),
            pltpu.VMEM((tok_rows, 1), jnp.int32),
            pltpu.SemaphoreType.DMA((2,)),
            pltpu.SemaphoreType.DMA((3,)),
            pltpu.SemaphoreType.DMA((groups,)),
            pltpu.SemaphoreType.DMA((groups,)),
            pltpu.SemaphoreType.DMA,
        ],
        compiler_params=pltpu.CompilerParams(
            collective_id=1, has_side_effects=True, vmem_limit_bytes=56 * 1024 * 1024
        ),
    )(
        tokens,
        expert_ids.reshape(1, tok_rows),
        norm_gain.reshape(1, width),
        weight_in,
        weight_out,
    )
    wide = tokens.astype(jnp.float32)
    mixed = (wide + gate_prob[:, None] * back.astype(jnp.float32)).astype(jnp.bfloat16)
    return mixed


def on_device(rows, cols, *args):
    mixed, routed, over = packed_layer(rows, cols, *args)
    mixed = lax.cond(
        over[0] > 0, lambda given, *all_args: slotted_layer(rows, cols, *all_args),
        lambda given, *all_args: given, mixed, *args,
    )
    return (mixed, routed)


def solution(mesh):
    return jax.shard_map(
        functools.partial(on_device, mesh.shape["row"], mesh.shape["col"]),
        mesh=mesh,
        in_specs=(
            P(("row", "col"), None),
            P(("row", "col"), None),
            P(("row", "col")),
            P(),
            P(("row", "col"), None, None),
            P(("row", "col"), None, None),
        ),
        out_specs=(P(("row", "col"), None), P(("row", "col"))),
        check_vma=False,
    )
```

```python
import functools

import jax
import jax.numpy as jnp
from jax import lax
from jax.experimental import pallas as pl
from jax.experimental.pallas import tpu as pltpu
from jax.sharding import PartitionSpec as P

MESH = pl.DeviceIdType.MESH


def bit_xor(a, b, size):
    out, unit = 0, 1
    while unit < size:
        out = out + lax.rem(lax.div(a, unit) + lax.div(b, unit), 2) * unit
        unit *= 2
    return out


def kernel(
    rows, cols, cap, groups, ff_tile, out_tile,
    tokens_ref, ids_row_ref, gain_ref, first_hbm, second_hbm,
    back_ref, routed_ref,
    first, second, normed, outgoing, received, answers, returned, hidden, total,
    counts, counts_in, placed_col,
    weight_sem, send_sem, recv_sem, ret_sem, count_sem,
):
    n = rows * cols
    tok_rows, width = tokens_ref.shape
    lanes = counts.shape[1]
    per = n // groups
    span = per * cap
    my_row, my_col = lax.axis_index("row"), lax.axis_index("col")
    me = my_row * cols + my_col

    def turn(step):
        if groups % 2:
            return step
        return lax.rem(step, 2) * (groups // 2) + lax.div(step, 2)

    def partner(place):
        q = n - 1 - place
        return (
            bit_xor(my_row, lax.rem(q, rows), rows),
            bit_xor(my_col, lax.div(q, rows), cols),
        )

    barrier = pltpu.get_barrier_semaphore()

    @pl.loop(0, n - 1)
    def _(place):
        pl.semaphore_signal(barrier, inc=1, device_id=partner(place), device_id_type=MESH)

    load_first = pltpu.make_async_copy(first_hbm.at[0], first, weight_sem.at[0])
    load_second = pltpu.make_async_copy(second_hbm.at[0], second, weight_sem.at[1])
    load_first.start()
    load_second.start()

    def slot_of(ids, within):
        offset = jnp.bitwise_xor(ids, me)
        q = (offset % cols) * rows + offset // cols
        return (n - 1 - q) * cap + within

    ids_row = ids_row_ref[...]
    at_row = lax.broadcasted_iota(jnp.int32, (tok_rows, tok_rows), 0)
    at_col = lax.broadcasted_iota(jnp.int32, (tok_rows, tok_rows), 1)
    hot_row = lax.broadcasted_iota(jnp.int32, (lanes, tok_rows), 0) == ids_row
    before = jnp.where(at_row < at_col, 1.0, 0.0).astype(jnp.bfloat16)
    earlier = jnp.dot(
        jnp.where(hot_row, 1.0, 0.0).astype(jnp.bfloat16), before, preferred_element_type=jnp.float32
    )
    within_row = jnp.sum(jnp.where(hot_row, earlier, 0.0), axis=0, keepdims=True)
    placed_row = slot_of(ids_row, within_row.astype(jnp.int32))

    wide = tokens_ref[...].astype(jnp.float32)
    scale = lax.rsqrt(jnp.mean(wide * wide, axis=1, keepdims=True) + 1e-06)
    normed[...] = (wide * scale * gain_ref[...]).astype(jnp.bfloat16)

    def as_blocks(values):
        return values.reshape(per, cap, width).astype(jnp.bfloat16)

    def as_rows(ref, g):
        blocks = ref[pl.ds(g * per, per)]
        if cap % 16 == 0:
            return blocks.reshape(span, width)
        return blocks.astype(jnp.float32).reshape(span, width).astype(jnp.bfloat16)

    def exchange(source, target, sem, out_sem, g):
        @pl.loop(0, per)
        def _(i):
            place = g * per + i

            @pl.when(place < n - 1)
            def _():
                pltpu.make_async_remote_copy(
                    src_ref=source.at[place],
                    dst_ref=target.at[place],
                    send_sem=out_sem,
                    recv_sem=sem.at[g],
                    device_id=partner(place),
                    device_id_type=MESH,
                ).start()

            @pl.when(place == n - 1)
            def _():
                pltpu.make_async_copy(source.at[n - 1], target.at[n - 1], sem.at[g]).start()

    def wait_group(target, sem, g):
        whole = target.at[pl.ds(g * per, per)]
        pltpu.make_async_copy(whole, whole, sem.at[g]).wait()

    @pl.loop(0, groups)
    def _(step):
        g = turn(step)
        slot = lax.broadcasted_iota(jnp.int32, (span, tok_rows), 0) + g * span
        table = jnp.where(slot == placed_row, 1.0, 0.0).astype(jnp.bfloat16)
        outgoing[pl.ds(g * per, per)] = as_blocks(
            jnp.dot(table, normed[...], preferred_element_type=jnp.float32)
        )

        @pl.when(step == 0)
        def _():
            pl.semaphore_wait(barrier, n - 1)

        exchange(outgoing, received, recv_sem, send_sem.at[0], g)

    counts[...] = lax.dot_general(
        jnp.ones((8, tok_rows), jnp.bfloat16),
        jnp.where(hot_row, 1.0, 0.0).astype(jnp.bfloat16),
        (((1,), (1,)), ((), ())),
        preferred_element_type=jnp.float32,
    )[0:1]
    turned = jnp.where(at_row == at_col, placed_row.astype(jnp.float32), 0.0)
    placed_col[...] = jnp.sum(turned, axis=1, keepdims=True).astype(jnp.int32)
    total[...] = jnp.zeros_like(total)

    @pl.loop(0, n - 1)
    def _(place):
        pltpu.make_async_remote_copy(
            src_ref=counts,
            dst_ref=counts_in.at[place],
            send_sem=send_sem.at[2],
            recv_sem=count_sem,
            device_id=partner(place),
            device_id_type=MESH,
        ).start()

    load_first.wait()
    load_second.wait()

    @pl.loop(0, groups)
    def _(step):
        g = turn(lax.rem(step + groups - 1, groups))
        wait_group(received, recv_sem, g)
        slab = as_rows(received, g)

        @pl.loop(0, first.shape[1] // ff_tile)
        def _(i):
            part = pl.ds(pl.multiple_of(i * ff_tile, ff_tile), ff_tile)
            grown = jnp.dot(slab, first[:, part], preferred_element_type=jnp.float32)
            hidden[:, part] = jnp.maximum(grown, 0.0).astype(jnp.bfloat16)

        @pl.loop(0, width // out_tile)
        def _(i):
            part = pl.ds(pl.multiple_of(i * out_tile, out_tile), out_tile)
            made = jnp.dot(hidden[...], second[:, part], preferred_element_type=jnp.float32)
            answers[pl.ds(g * per, per), :, part] = made.reshape(per, cap, out_tile).astype(
                jnp.bfloat16
            )

        exchange(answers, returned, ret_sem, send_sem.at[1], g)

    arrived = counts_in.at[pl.ds(0, n - 1)]
    pltpu.make_async_copy(arrived, arrived, count_sem).wait()
    sums = jnp.sum(counts_in[pl.ds(0, n - 1)], axis=0) + counts[...]
    mine = lax.broadcasted_iota(jnp.int32, (1, lanes), 1) == me
    routed_ref[0] = jnp.sum(jnp.where(mine, sums, 0.0)).astype(jnp.int32)

    @pl.loop(0, groups)
    def _(step):
        g = turn(lax.rem(step + groups - 1, groups))
        wait_group(returned, ret_sem, g)
        slot = lax.broadcasted_iota(jnp.int32, (tok_rows, span), 1) + g * span
        table = jnp.where(slot == placed_col[...], 1.0, 0.0).astype(jnp.bfloat16)
        total[...] += jnp.dot(table, as_rows(returned, g), preferred_element_type=jnp.float32)

    back_ref[...] = total[...].astype(jnp.bfloat16)

    sent = outgoing.at[pl.ds(0, n - 1)]
    pltpu.make_async_copy(sent, sent, send_sem.at[0]).wait()
    pltpu.make_async_copy(sent, sent, send_sem.at[1]).wait()
    pltpu.make_async_copy(arrived, arrived, send_sem.at[2]).wait()


def flipped(a, mask, size):
    out, unit = 0, 1
    while unit < size:
        bit = lax.rem(lax.div(a, unit), 2)
        out = out + ((1 - bit) if (mask // unit) % 2 else bit) * unit
        unit *= 2
    return out


def packed_kernel(
    rows, cols, low, cap, keep, parts, ff_tile, out_tile,
    tokens_hbm, ids_hbm, gate_hbm, gain_hbm, first_hbm, second_hbm,
    mixed_hbm, routed_ref, over_ref,
    tokens_ref, ids_row_ref, gate_row_ref, gain_ref, mixed_ref, first, second, normed, packed, packed_in, slots, slots_in, answers, answers_in,
    back, back_in, hidden, total, counts, counts_far, sums, sums_in,
    index_row, index_col, placed_col, gate_col,
    load_sem, store_sem, send_sem, far_sem, near_sem, answer_sem, back_sem, count_sem,
):
    n = rows * cols
    planes = cols // low
    per = n // planes
    span = per * cap
    tok_rows, width = tokens_ref.shape
    wide_part = width // parts
    lanes = counts.shape[1]
    my_row, my_col = lax.axis_index("row"), lax.axis_index("col")
    me = my_row * cols + my_col
    row_at = [flipped(my_row, c, rows) for c in range(rows)]
    low_at = [flipped(lax.rem(my_col, low), c, low) for c in range(low)]
    plane_at = [flipped(lax.div(my_col, low), c, planes) * low for c in range(planes)]
    far = list(range(planes - 1, 0, -1))
    half = planes // 2
    sent = [planes - 1 - k for i in range(half) for k in (i, i + half)][: planes - 1]
    if planes % 2:
        sent = far

    def device(k, j):
        return (row_at[j % rows], plane_at[k] + low_at[j // rows])

    def send(source, target, out_sem, sem, where):
        pltpu.make_async_remote_copy(
            src_ref=source, dst_ref=target, send_sem=out_sem, recv_sem=sem,
            device_id=where, device_id_type=MESH,
        ).start()

    def wait(ref, sem, name="wait_last"):
        with jax.named_scope(name):
            pltpu.make_async_copy(ref, ref, sem).wait()

    barrier = pltpu.get_barrier_semaphore()
    near_by = [(0, j) for j in range(1, per)]
    peers = [(k, 0) for k in far] + near_by
    for k, j in peers:
        pl.semaphore_signal(barrier, inc=1, device_id=device(k, j), device_id_type=MESH)

    loads = [
        pltpu.make_async_copy(source, target, load_sem.at[i])
        for i, (source, target) in enumerate(
            (
                (ids_hbm, ids_row_ref), (tokens_hbm, tokens_ref), (gain_hbm, gain_ref),
                (gate_hbm, gate_row_ref), (first_hbm.at[0], first), (second_hbm.at[0], second),
            )
        )
    ]
    for load in loads:
        load.start()
    loads[0].wait()

    def place_of(ids):
        offset = jnp.bitwise_xor(ids, me)
        return (offset % cols) // low, offset // cols + rows * (offset % low)

    def ones_at(condition):
        return jnp.where(condition, 1.0, 0.0).astype(jnp.bfloat16)

    ids_row = ids_row_ref[...]
    at_row = lax.broadcasted_iota(jnp.int32, (tok_rows, tok_rows), 0)
    at_col = lax.broadcasted_iota(jnp.int32, (tok_rows, tok_rows), 1)
    hot = lax.broadcasted_iota(jnp.int32, (lanes, tok_rows), 0) == ids_row
    hot_bf = ones_at(hot)
    earlier = jnp.dot(hot_bf, ones_at(at_row < at_col), preferred_element_type=jnp.float32)
    within = jnp.sum(jnp.where(hot, earlier, 0.0), axis=0, keepdims=True)
    plane_e, near_e = place_of(lax.broadcasted_iota(jnp.int32, (lanes, 1), 0))
    plane_t, near_t = place_of(ids_row)
    count_e = jnp.sum(jnp.where(hot, 1.0, 0.0), axis=1, keepdims=True)
    sooner = (plane_e == plane_t) & (near_e < near_t)
    ahead = jnp.sum(jnp.where(sooner, count_e, 0.0), axis=0, keepdims=True)
    start = jnp.where(plane_t == 0, near_t * cap, ahead.astype(jnp.int32))
    placed_row = plane_t * span + start + within.astype(jnp.int32)

    loads[1].wait()
    loads[2].wait()
    wide = tokens_ref[...].astype(jnp.float32)
    scale = lax.rsqrt(jnp.mean(wide * wide, axis=1, keepdims=True) + 1e-06)
    normed[...] = (wide * scale * gain_ref[...]).astype(jnp.bfloat16)

    tally = lax.dot_general(
        jnp.ones((8, tok_rows), jnp.bfloat16), hot_bf,
        (((1,), (1,)), ((), ())), preferred_element_type=jnp.float32,
    )[0:1]
    lane = lax.broadcasted_iota(jnp.int32, (1, lanes), 1)
    plane_l, _ = place_of(lane)
    over = jnp.zeros((1, 1), jnp.float32)
    for k in far:
        held = jnp.sum(jnp.where(plane_l == k, tally, 0.0), axis=1, keepdims=True)
        over = over + jnp.where(held > keep, 1.0, 0.0)
    counts[...] = tally + jnp.where(lane == n, over, 0.0)

    def columns(h):
        return pl.ds(h * wide_part, wide_part)

    def gather_from(k, size):
        slot = lax.broadcasted_iota(jnp.int32, (size, tok_rows), 0) + k * span
        return ones_at(slot == placed_row)

    def pack(k):
        table = gather_from(k, keep)
        for h in range(parts):
            packed[k, h] = jnp.dot(
                table, normed[:, columns(h)], preferred_element_type=jnp.float32
            ).astype(jnp.bfloat16)

    def send_far(k):
        for h in range(parts):
            send(packed.at[k, h], packed_in.at[k, h], send_sem.at[0], far_sem.at[k, h], device(k, 0))

    def send_near(source, target, out_sem, sem, k, h):
        for j in range(1, per):
            block = pl.ds(j * cap, cap)
            send(
                source.at[k, h, block], target.at[k, h, block], out_sem, sem.at[k, h], device(0, j)
            )

    def wait_near(target, sem, k, h, name):
        wait(target.at[k, h, pl.ds(cap, span - cap)], sem.at[k, h], f"{name}#k={k}#h={h}")

    def fill(k, h, values):
        made = values.astype(jnp.bfloat16)
        slots_in[k, h, 0:cap] = made[0:cap]
        slots[k, h] = made
        send_near(slots, slots_in, send_sem.at[1], near_sem, k, h)

    pack(far[0])
    with jax.named_scope("barrier_wait"):
        pl.semaphore_wait(barrier, len(peers))
    for k in far:
        send(counts, counts_far.at[k], send_sem.at[4], count_sem.at[0], device(k, 0))
    send_far(far[0])
    table = gather_from(0, span)
    for h in range(parts):
        fill(0, h, jnp.dot(table, normed[:, columns(h)], preferred_element_type=jnp.float32))
    for k in sent[1:]:
        pack(k)
        send_far(k)
    def to_column(row, size):
        there = lax.broadcasted_iota(jnp.int32, (size, size), 0)
        here = lax.broadcasted_iota(jnp.int32, (size, size), 1)
        return jnp.sum(jnp.where(there == here, row, 0.0), axis=1, keepdims=True)

    placed_col[...] = to_column(placed_row.astype(jnp.float32), tok_rows).astype(jnp.int32)
    loads[3].wait()
    gate_col[...] = to_column(gate_row_ref[...], tok_rows)

    wait(counts_far.at[pl.ds(1, planes - 1)], count_sem.at[0], "wait_counts")
    sums[...] = counts[...] + jnp.sum(counts_far[pl.ds(1, planes - 1)], axis=0)
    for k, j in near_by:
        send(sums, sums_in.at[j], send_sem.at[5], count_sem.at[1], device(k, j))
    expert = lax.broadcasted_iota(jnp.int32, (lanes, span), 0)
    plane_s, near_s = place_of(expert)
    here = (plane_s == 0) & (expert < n)
    slot = lax.broadcasted_iota(jnp.int32, (lanes, span), 1)
    at_block = ones_at(here & (near_s == slot // cap))
    before_block = ones_at(here & (near_s < slot // cap))
    slot_row = lax.broadcasted_iota(jnp.int32, (1, span), 1)
    rank = (slot_row % cap).astype(jnp.float32)
    for k in far:
        tall = jnp.broadcast_to(counts_far[k], (8, lanes)).astype(jnp.bfloat16)
        held = jnp.dot(tall, at_block, preferred_element_type=jnp.float32)[0:1]
        begin = jnp.dot(tall, before_block, preferred_element_type=jnp.float32)[0:1]
        index = jnp.where(rank < held, begin + rank, -1.0)
        index_row[k] = index.astype(jnp.int32)
        index_col[k] = to_column(index, span).astype(jnp.int32)

    with jax.named_scope("wait_weights"):
        loads[4].wait()
        loads[5].wait()

    def relay(k, h):
        wait(packed_in.at[k, h], far_sem.at[k, h], f"wait_far#k={k}#h={h}")
        slot = lax.broadcasted_iota(jnp.int32, (span, keep), 1)
        table = ones_at(slot == index_col[k])
        fill(k, h, jnp.dot(table, packed_in[k, h], preferred_element_type=jnp.float32))

    def await_slots(k):
        for h in range(parts):
            wait_near(slots_in, near_sem, k, h, "wait_slots")

    def grow(k):
        @pl.loop(0, first.shape[1] // ff_tile, unroll=min(4, first.shape[1] // ff_tile))
        def _(i):
            part = pl.ds(pl.multiple_of(i * ff_tile, ff_tile), ff_tile)
            grown = jnp.dot(slots_in[k, 0], first[columns(0), part], preferred_element_type=jnp.float32)
            for h in range(1, parts):
                grown += jnp.dot(
                    slots_in[k, h], first[columns(h), part], preferred_element_type=jnp.float32
                )
            hidden[:, part] = jnp.maximum(grown, 0.0).astype(jnp.bfloat16)

    def shrink(k, h):
        @pl.loop(0, wide_part // out_tile, unroll=True)
        def _(i):
            at = pl.multiple_of(i * out_tile, out_tile)
            part = pl.ds(pl.multiple_of(h * wide_part + i * out_tile, out_tile), out_tile)
            made = jnp.dot(hidden[...], second[:, part], preferred_element_type=jnp.float32)
            made = made.astype(jnp.bfloat16)
            answers[k, h, :, pl.ds(at, out_tile)] = made
            answers_in[k, h, 0:cap, pl.ds(at, out_tile)] = made[0:cap]

    def send_answers(k, h):
        send_near(answers, answers_in, send_sem.at[2], answer_sem, k, h)

    def give_back(k, h):
        wait_near(answers_in, answer_sem, k, h, "wait_answers")
        slot = lax.broadcasted_iota(jnp.int32, (keep, span), 0)
        table = ones_at(slot == index_row[k])
        back[k, h] = jnp.dot(
            table, answers_in[k, h], preferred_element_type=jnp.float32
        ).astype(jnp.bfloat16)
        send(back.at[k, h], back_in.at[k, h], send_sem.at[3], back_sem.at[k, h], device(k, 0))

    def picked(k, h):
        size = keep if k else span
        if k:
            wait(back_in.at[k, h], back_sem.at[k, h], f"wait_back#k={k}#h={h}")
        else:
            wait_near(answers_in, answer_sem, 0, h, "wait_answers")
        source = back_in if k else answers_in
        slot = lax.broadcasted_iota(jnp.int32, (tok_rows, size), 1) + k * span
        table = ones_at(slot == placed_col[...])
        return jnp.dot(table, source[k, h], preferred_element_type=jnp.float32)

    halves = range(parts)
    todo = far[:1] + far[:0:-1]
    await_slots(0)
    grow(0)
    for h in halves:
        shrink(0, h)
    for k in todo[:2]:
        for h in halves:
            relay(k, h)
    for i, k in enumerate(todo):
        await_slots(k)
        grow(k)
        for k2 in todo[i + 1 : i + 2] if i else []:
            for h in halves:
                relay(k2, h)
        for h in halves:
            if i == 1:
                give_back(todo[0], h)
        for h in halves:
            shrink(k, h)
            send_answers(k, h)
            if i > 1:
                give_back(todo[i - 1], h)
    for h in halves:
        give_back(todo[-1], h)
    for h in halves:
        send_answers(0, h)

    wait(sums_in.at[pl.ds(1, per - 1)], count_sem.at[1])
    whole = sums[...] + jnp.sum(sums_in[pl.ds(1, per - 1)], axis=0)
    routed_ref[0] = jnp.sum(jnp.where(lane == me, whole, 0.0)).astype(jnp.int32)
    over_ref[0] = jnp.sum(jnp.where(lane == n, whole, 0.0)).astype(jnp.int32)

    for h in range(parts):
        total[h] = picked(0, h)
    for k in todo[:-1]:
        for h in range(parts):
            total[h] += picked(k, h)
    for h in range(parts):
        found = total[h] + picked(todo[-1], h)
        kept = tokens_ref[:, columns(h)].astype(jnp.float32)
        mixed_ref[:, columns(h)] = (kept + gate_col[...] * found).astype(jnp.bfloat16)
        pltpu.make_async_copy(
            mixed_ref.at[:, columns(h)], mixed_hbm.at[:, columns(h)], store_sem.at[h]
        ).start()

    wait(packed.at[pl.ds(1, planes - 1)], send_sem.at[0])
    wait(slots.at[:, :, pl.ds(cap, span - cap)], send_sem.at[1])
    wait(answers.at[:, :, pl.ds(cap, span - cap)], send_sem.at[2])
    wait(back.at[pl.ds(1, planes - 1)], send_sem.at[3])
    wait(counts_far.at[pl.ds(1, planes - 1)], send_sem.at[4])
    wait(sums_in.at[pl.ds(1, per - 1)], send_sem.at[5])
    for h in halves:
        wait(mixed_ref.at[:, columns(h)], store_sem.at[h])


def packed_layer(rows, cols, tokens, expert_ids, gate_prob, norm_gain, weight_in, weight_out):
    tok_rows, width = tokens.shape
    hidden_width = weight_in.shape[2]
    n = rows * cols
    low = min(2, cols)
    planes = cols // low
    per = n // planes
    cap = 2 * tok_rows // n
    span = per * cap
    keep = 3 * span // 4
    parts = 2
    part = width // parts
    lanes = -(-(n + 1) // 128) * 128
    smem = pl.BlockSpec(memory_space=pltpu.SMEM)
    hbm = pl.BlockSpec(memory_space=pl.ANY)
    tight = pltpu.VMEM((planes, parts, keep, part), jnp.bfloat16)
    loose = pltpu.VMEM((planes, parts, span, part), jnp.bfloat16)
    each = pltpu.SemaphoreType.DMA((planes, parts))
    return pl.pallas_call(
        functools.partial(
            packed_kernel, rows, cols, low, cap, keep, parts,
            min(512, hidden_width), min(256, part),
        ),
        out_shape=(
            jax.ShapeDtypeStruct((tok_rows, width), jnp.bfloat16),
            jax.ShapeDtypeStruct((1,), jnp.int32),
            jax.ShapeDtypeStruct((1,), jnp.int32),
        ),
        in_specs=[hbm, hbm, hbm, hbm, hbm, hbm],
        out_specs=(hbm, smem, smem),
        scratch_shapes=[
            pltpu.VMEM((tok_rows, width), jnp.bfloat16),
            pltpu.VMEM((1, tok_rows), jnp.int32),
            pltpu.VMEM((1, tok_rows), jnp.float32),
            pltpu.VMEM((1, width), jnp.float32),
            pltpu.VMEM((tok_rows, width), jnp.bfloat16),
            pltpu.VMEM((width, hidden_width), jnp.bfloat16),
            pltpu.VMEM((hidden_width, width), jnp.bfloat16),
            pltpu.VMEM((tok_rows, width), jnp.bfloat16),
            tight, tight, loose, loose, loose, loose, tight, tight,
            pltpu.VMEM((span, hidden_width), jnp.bfloat16),
            pltpu.VMEM((parts, tok_rows, part), jnp.float32),
            pltpu.VMEM((1, lanes), jnp.float32),
            pltpu.VMEM((planes, 1, lanes), jnp.float32),
            pltpu.VMEM((1, lanes), jnp.float32),
            pltpu.VMEM((per, 1, lanes), jnp.float32),
            pltpu.VMEM((planes, 1, span), jnp.int32),
            pltpu.VMEM((planes, span, 1), jnp.int32),
            pltpu.VMEM((tok_rows, 1), jnp.int32),
            pltpu.VMEM((tok_rows, 1), jnp.float32),
            pltpu.SemaphoreType.DMA((6,)),
            pltpu.SemaphoreType.DMA((parts,)),
            pltpu.SemaphoreType.DMA((6,)),
            each, each, each, each,
            pltpu.SemaphoreType.DMA((2,)),
        ],
        compiler_params=pltpu.CompilerParams(
            collective_id=0, has_side_effects=True, vmem_limit_bytes=56 * 1024 * 1024
        ),
    )(
        tokens,
        expert_ids.reshape(1, tok_rows),
        gate_prob.reshape(1, tok_rows),
        norm_gain.reshape(1, width),
        weight_in,
        weight_out,
    )


def slotted_layer(rows, cols, tokens, expert_ids, gate_prob, norm_gain, weight_in, weight_out):
    tok_rows, width = tokens.shape
    hidden_width = weight_in.shape[2]
    n = rows * cols
    cap = 2 * tok_rows // n
    lanes = -(-n // 128) * 128
    per = max(1, min(n, 256 // cap))
    groups = n // per
    vmem = pl.BlockSpec(memory_space=pltpu.VMEM)
    hbm = pl.BlockSpec(memory_space=pl.ANY)
    block = pltpu.VMEM((n, cap, width), jnp.bfloat16)
    back, routed = pl.pallas_call(
        functools.partial(kernel, rows, cols, cap, groups, min(512, hidden_width), min(256, width)),
        out_shape=(
            jax.ShapeDtypeStruct((tok_rows, width), jnp.bfloat16),
            jax.ShapeDtypeStruct((1,), jnp.int32),
        ),
        in_specs=[vmem, vmem, vmem, hbm, hbm],
        out_specs=(vmem, pl.BlockSpec(memory_space=pltpu.SMEM)),
        scratch_shapes=[
            pltpu.VMEM((width, hidden_width), jnp.bfloat16),
            pltpu.VMEM((hidden_width, width), jnp.bfloat16),
            pltpu.VMEM((tok_rows, width), jnp.bfloat16),
            block, block, block, block,
            pltpu.VMEM((per * cap, hidden_width), jnp.bfloat16),
            pltpu.VMEM((tok_rows, width), jnp.float32),
            pltpu.VMEM((1, lanes), jnp.float32),
            pltpu.VMEM((n, 1, lanes), jnp.float32),
            pltpu.VMEM((tok_rows, 1), jnp.int32),
            pltpu.SemaphoreType.DMA((2,)),
            pltpu.SemaphoreType.DMA((3,)),
            pltpu.SemaphoreType.DMA((groups,)),
            pltpu.SemaphoreType.DMA((groups,)),
            pltpu.SemaphoreType.DMA,
        ],
        compiler_params=pltpu.CompilerParams(
            collective_id=1, has_side_effects=True, vmem_limit_bytes=56 * 1024 * 1024
        ),
    )(
        tokens,
        expert_ids.reshape(1, tok_rows),
        norm_gain.reshape(1, width),
        weight_in,
        weight_out,
    )
    wide = tokens.astype(jnp.float32)
    mixed = (wide + gate_prob[:, None] * back.astype(jnp.float32)).astype(jnp.bfloat16)
    return mixed


def on_device(rows, cols, *args):
    mixed, routed, over = packed_layer(rows, cols, *args)
    mixed = lax.cond(
        over[0] > 0, lambda given, *all_args: slotted_layer(rows, cols, *all_args),
        lambda given, *all_args: given, mixed, *args,
    )
    return (mixed, routed)


def solution(mesh):
    return jax.shard_map(
        functools.partial(on_device, mesh.shape["row"], mesh.shape["col"]),
        mesh=mesh,
        in_specs=(
            P(("row", "col"), None),
            P(("row", "col"), None),
            P(("row", "col")),
            P(),
            P(("row", "col"), None, None),
            P(("row", "col"), None, None),
        ),
        out_specs=(P(("row", "col"), None), P(("row", "col"))),
        check_vma=False,
    )
```

```python
import functools

import jax
import jax.numpy as jnp
from jax import lax
from jax.experimental import pallas as pl
from jax.experimental.pallas import tpu as pltpu
from jax.sharding import PartitionSpec as P

MESH = pl.DeviceIdType.MESH


def bit_xor(a, b, size):
    out, unit = 0, 1
    while unit < size:
        out = out + lax.rem(lax.div(a, unit) + lax.div(b, unit), 2) * unit
        unit *= 2
    return out


def kernel(
    rows, cols, cap, groups, ff_tile, out_tile,
    tokens_ref, ids_row_ref, gain_ref, first_hbm, second_hbm,
    back_ref, routed_ref,
    first, second, normed, outgoing, received, answers, returned, hidden, total,
    counts, counts_in, placed_col,
    weight_sem, send_sem, recv_sem, ret_sem, count_sem,
):
    n = rows * cols
    tok_rows, width = tokens_ref.shape
    lanes = counts.shape[1]
    per = n // groups
    span = per * cap
    my_row, my_col = lax.axis_index("row"), lax.axis_index("col")
    me = my_row * cols + my_col

    def turn(step):
        if groups % 2:
            return step
        return lax.rem(step, 2) * (groups // 2) + lax.div(step, 2)

    def partner(place):
        q = n - 1 - place
        return (
            bit_xor(my_row, lax.rem(q, rows), rows),
            bit_xor(my_col, lax.div(q, rows), cols),
        )

    barrier = pltpu.get_barrier_semaphore()

    @pl.loop(0, n - 1)
    def _(place):
        pl.semaphore_signal(barrier, inc=1, device_id=partner(place), device_id_type=MESH)

    load_first = pltpu.make_async_copy(first_hbm.at[0], first, weight_sem.at[0])
    load_second = pltpu.make_async_copy(second_hbm.at[0], second, weight_sem.at[1])
    load_first.start()
    load_second.start()

    def slot_of(ids, within):
        offset = jnp.bitwise_xor(ids, me)
        q = (offset % cols) * rows + offset // cols
        return (n - 1 - q) * cap + within

    ids_row = ids_row_ref[...]
    at_row = lax.broadcasted_iota(jnp.int32, (tok_rows, tok_rows), 0)
    at_col = lax.broadcasted_iota(jnp.int32, (tok_rows, tok_rows), 1)
    hot_row = lax.broadcasted_iota(jnp.int32, (lanes, tok_rows), 0) == ids_row
    before = jnp.where(at_row < at_col, 1.0, 0.0).astype(jnp.bfloat16)
    earlier = jnp.dot(
        jnp.where(hot_row, 1.0, 0.0).astype(jnp.bfloat16), before, preferred_element_type=jnp.float32
    )
    within_row = jnp.sum(jnp.where(hot_row, earlier, 0.0), axis=0, keepdims=True)
    placed_row = slot_of(ids_row, within_row.astype(jnp.int32))

    wide = tokens_ref[...].astype(jnp.float32)
    scale = lax.rsqrt(jnp.mean(wide * wide, axis=1, keepdims=True) + 1e-06)
    normed[...] = (wide * scale * gain_ref[...]).astype(jnp.bfloat16)

    def as_blocks(values):
        return values.reshape(per, cap, width).astype(jnp.bfloat16)

    def as_rows(ref, g):
        blocks = ref[pl.ds(g * per, per)]
        if cap % 16 == 0:
            return blocks.reshape(span, width)
        return blocks.astype(jnp.float32).reshape(span, width).astype(jnp.bfloat16)

    def exchange(source, target, sem, out_sem, g):
        @pl.loop(0, per)
        def _(i):
            place = g * per + i

            @pl.when(place < n - 1)
            def _():
                pltpu.make_async_remote_copy(
                    src_ref=source.at[place],
                    dst_ref=target.at[place],
                    send_sem=out_sem,
                    recv_sem=sem.at[g],
                    device_id=partner(place),
                    device_id_type=MESH,
                ).start()

            @pl.when(place == n - 1)
            def _():
                pltpu.make_async_copy(source.at[n - 1], target.at[n - 1], sem.at[g]).start()

    def wait_group(target, sem, g):
        whole = target.at[pl.ds(g * per, per)]
        pltpu.make_async_copy(whole, whole, sem.at[g]).wait()

    @pl.loop(0, groups)
    def _(step):
        g = turn(step)
        slot = lax.broadcasted_iota(jnp.int32, (span, tok_rows), 0) + g * span
        table = jnp.where(slot == placed_row, 1.0, 0.0).astype(jnp.bfloat16)
        outgoing[pl.ds(g * per, per)] = as_blocks(
            jnp.dot(table, normed[...], preferred_element_type=jnp.float32)
        )

        @pl.when(step == 0)
        def _():
            pl.semaphore_wait(barrier, n - 1)

        exchange(outgoing, received, recv_sem, send_sem.at[0], g)

    counts[...] = lax.dot_general(
        jnp.ones((8, tok_rows), jnp.bfloat16),
        jnp.where(hot_row, 1.0, 0.0).astype(jnp.bfloat16),
        (((1,), (1,)), ((), ())),
        preferred_element_type=jnp.float32,
    )[0:1]
    turned = jnp.where(at_row == at_col, placed_row.astype(jnp.float32), 0.0)
    placed_col[...] = jnp.sum(turned, axis=1, keepdims=True).astype(jnp.int32)
    total[...] = jnp.zeros_like(total)

    @pl.loop(0, n - 1)
    def _(place):
        pltpu.make_async_remote_copy(
            src_ref=counts,
            dst_ref=counts_in.at[place],
            send_sem=send_sem.at[2],
            recv_sem=count_sem,
            device_id=partner(place),
            device_id_type=MESH,
        ).start()

    load_first.wait()
    load_second.wait()

    @pl.loop(0, groups)
    def _(step):
        g = turn(lax.rem(step + groups - 1, groups))
        wait_group(received, recv_sem, g)
        slab = as_rows(received, g)

        @pl.loop(0, first.shape[1] // ff_tile)
        def _(i):
            part = pl.ds(pl.multiple_of(i * ff_tile, ff_tile), ff_tile)
            grown = jnp.dot(slab, first[:, part], preferred_element_type=jnp.float32)
            hidden[:, part] = jnp.maximum(grown, 0.0).astype(jnp.bfloat16)

        @pl.loop(0, width // out_tile)
        def _(i):
            part = pl.ds(pl.multiple_of(i * out_tile, out_tile), out_tile)
            made = jnp.dot(hidden[...], second[:, part], preferred_element_type=jnp.float32)
            answers[pl.ds(g * per, per), :, part] = made.reshape(per, cap, out_tile).astype(
                jnp.bfloat16
            )

        exchange(answers, returned, ret_sem, send_sem.at[1], g)

    arrived = counts_in.at[pl.ds(0, n - 1)]
    pltpu.make_async_copy(arrived, arrived, count_sem).wait()
    sums = jnp.sum(counts_in[pl.ds(0, n - 1)], axis=0) + counts[...]
    mine = lax.broadcasted_iota(jnp.int32, (1, lanes), 1) == me
    routed_ref[0] = jnp.sum(jnp.where(mine, sums, 0.0)).astype(jnp.int32)

    @pl.loop(0, groups)
    def _(step):
        g = turn(lax.rem(step + groups - 1, groups))
        wait_group(returned, ret_sem, g)
        slot = lax.broadcasted_iota(jnp.int32, (tok_rows, span), 1) + g * span
        table = jnp.where(slot == placed_col[...], 1.0, 0.0).astype(jnp.bfloat16)
        total[...] += jnp.dot(table, as_rows(returned, g), preferred_element_type=jnp.float32)

    back_ref[...] = total[...].astype(jnp.bfloat16)

    sent = outgoing.at[pl.ds(0, n - 1)]
    pltpu.make_async_copy(sent, sent, send_sem.at[0]).wait()
    pltpu.make_async_copy(sent, sent, send_sem.at[1]).wait()
    pltpu.make_async_copy(arrived, arrived, send_sem.at[2]).wait()


def flipped(a, mask, size):
    out, unit = 0, 1
    while unit < size:
        bit = lax.rem(lax.div(a, unit), 2)
        out = out + ((1 - bit) if (mask // unit) % 2 else bit) * unit
        unit *= 2
    return out


def packed_kernel(
    rows, cols, low, cap, near_keep, main, pool, parts, ff_tile, out_tile,
    tokens_hbm, ids_hbm, gate_hbm, gain_hbm, first_hbm, second_hbm,
    mixed_hbm, routed_ref, over_ref,
    tokens_ref, ids_row_ref, gate_row_ref, gain_ref, mixed_ref, first, second, normed, packed, packed_in, slots, slots_in, answers, answers_in,
    back, back_in, pooled, pool_in, pool_out, pool_back, hidden, total, counts, counts_far, sums, sums_in,
    index_row, index_col, placed_col, gate_col,
    load_sem, store_sem, send_sem, far_sem, near_sem, answer_sem, back_sem, pool_sem, merge_sem, count_sem,
):
    n = rows * cols
    planes = cols // low
    per = n // planes
    span = per * cap
    tok_rows, width = tokens_ref.shape
    wide_part = width // parts
    lanes = counts.shape[1]
    my_row, my_col = lax.axis_index("row"), lax.axis_index("col")
    me = my_row * cols + my_col
    row_at = [flipped(my_row, c, rows) for c in range(rows)]
    low_at = [flipped(lax.rem(my_col, low), c, low) for c in range(low)]
    plane_at = [flipped(lax.div(my_col, low), c, planes) * low for c in range(planes)]
    far = list(range(planes - 1, 0, -1))
    half = planes // 2
    sent = [planes - 1 - k for i in range(half) for k in (i, i + half)][: planes - 1]
    if planes % 2:
        sent = far

    pairs = list(range(2, planes, 2))

    def keep_of(k):
        return near_keep if k == 1 else main

    def pool_row(rank, k):
        return pool - 1 - (rank - main) if k % 2 else rank - main

    def device(k, j):
        return (row_at[j % rows], plane_at[k] + low_at[j // rows])

    def send(source, target, out_sem, sem, where):
        pltpu.make_async_remote_copy(
            src_ref=source, dst_ref=target, send_sem=out_sem, recv_sem=sem,
            device_id=where, device_id_type=MESH,
        ).start()

    def wait(ref, sem, name="wait_last"):
        with jax.named_scope(name):
            pltpu.make_async_copy(ref, ref, sem).wait()

    barrier = pltpu.get_barrier_semaphore()
    near_by = [(0, j) for j in range(1, per)]
    peers = [(k, 0) for k in far] + near_by
    for k, j in peers:
        pl.semaphore_signal(barrier, inc=1, device_id=device(k, j), device_id_type=MESH)

    loads = [
        pltpu.make_async_copy(source, target, load_sem.at[i])
        for i, (source, target) in enumerate(
            (
                (ids_hbm, ids_row_ref), (tokens_hbm, tokens_ref), (gain_hbm, gain_ref),
                (gate_hbm, gate_row_ref), (first_hbm.at[0], first), (second_hbm.at[0], second),
            )
        )
    ]
    for load in loads:
        load.start()
    loads[0].wait()

    def place_of(ids):
        offset = jnp.bitwise_xor(ids, me)
        return (offset % cols) // low, offset // cols + rows * (offset % low)

    def ones_at(condition):
        return jnp.where(condition, 1.0, 0.0).astype(jnp.bfloat16)

    ids_row = ids_row_ref[...]
    at_row = lax.broadcasted_iota(jnp.int32, (tok_rows, tok_rows), 0)
    at_col = lax.broadcasted_iota(jnp.int32, (tok_rows, tok_rows), 1)
    hot = lax.broadcasted_iota(jnp.int32, (lanes, tok_rows), 0) == ids_row
    hot_bf = ones_at(hot)
    earlier = jnp.dot(hot_bf, ones_at(at_row < at_col), preferred_element_type=jnp.float32)
    within = jnp.sum(jnp.where(hot, earlier, 0.0), axis=0, keepdims=True)
    plane_e, near_e = place_of(lax.broadcasted_iota(jnp.int32, (lanes, 1), 0))
    plane_t, near_t = place_of(ids_row)
    count_e = jnp.sum(jnp.where(hot, 1.0, 0.0), axis=1, keepdims=True)
    sooner = (plane_e == plane_t) & (near_e < near_t)
    ahead = jnp.sum(jnp.where(sooner, count_e, 0.0), axis=0, keepdims=True)
    start = jnp.where(plane_t == 0, near_t * cap, ahead.astype(jnp.int32))
    placed_row = plane_t * span + start + within.astype(jnp.int32)

    loads[1].wait()
    loads[2].wait()
    wide = tokens_ref[...].astype(jnp.float32)
    scale = lax.rsqrt(jnp.mean(wide * wide, axis=1, keepdims=True) + 1e-06)
    normed[...] = (wide * scale * gain_ref[...]).astype(jnp.bfloat16)

    tally = lax.dot_general(
        jnp.ones((8, tok_rows), jnp.bfloat16), hot_bf,
        (((1,), (1,)), ((), ())), preferred_element_type=jnp.float32,
    )[0:1]
    lane = lax.broadcasted_iota(jnp.int32, (1, lanes), 1)
    plane_l, _ = place_of(lane)
    over = jnp.zeros((1, 1), jnp.float32)
    held = [jnp.sum(jnp.where(plane_l == k, tally, 0.0), axis=1, keepdims=True) for k in range(planes)]
    for k in far:
        if k == 1:
            over = over + jnp.where(held[1] > near_keep, 1.0, 0.0)
        elif k % 2 == 0:
            extra = jnp.maximum(held[k] - main, 0.0) + jnp.maximum(held[k + 1] - main, 0.0)
            over = over + jnp.where(extra > pool, 1.0, 0.0)
    counts[...] = tally + jnp.where(lane == n, over, 0.0)

    def columns(h):
        return pl.ds(h * wide_part, wide_part)

    def gather_from(k, size):
        slot = lax.broadcasted_iota(jnp.int32, (size, tok_rows), 0) + k * span
        return ones_at(slot == placed_row)

    def chunk(ref, k, h):
        return ref.at[k, h, pl.ds(0, keep_of(k))]

    def in_pool(slot, placed, k):
        first_hit = slot == pool_row(placed - k * span, k)
        return ones_at(first_hit | (slot == pool_row(placed - (k + 1) * span, k + 1)))

    def pack(k):
        table = gather_from(k, keep_of(k))
        for h in range(parts):
            packed[k, h, 0 : keep_of(k)] = jnp.dot(
                table, normed[:, columns(h)], preferred_element_type=jnp.float32
            ).astype(jnp.bfloat16)

    def pack_pool(k):
        slot = lax.broadcasted_iota(jnp.int32, (pool, tok_rows), 0)
        table = in_pool(slot, placed_row, k)
        for h in range(parts):
            pooled[k // 2, h] = jnp.dot(
                table, normed[:, columns(h)], preferred_element_type=jnp.float32
            ).astype(jnp.bfloat16)

    def send_far(k):
        for h in range(parts):
            send(
                chunk(packed, k, h), chunk(packed_in, k, h), send_sem.at[0 if k > 1 else 6],
                far_sem.at[k, h], device(k, 0),
            )
            if k > 1 and k % 2:
                send(
                    pooled.at[k // 2, h], pool_in.at[k, h], send_sem.at[7], pool_sem.at[k, h],
                    device(k, 0),
                )

    def pass_pool(k, h):
        send(
            pool_in.at[k, h], pool_in.at[k - 1, h], send_sem.at[8], pool_sem.at[k - 1, h],
            device(1, 0),
        )

    def send_near(source, target, out_sem, sem, k, h):
        for j in range(1, per):
            block = pl.ds(j * cap, cap)
            send(
                source.at[k, h, block], target.at[k, h, block], out_sem, sem.at[k, h], device(0, j)
            )

    def wait_near(target, sem, k, h, name):
        wait(target.at[k, h, pl.ds(cap, span - cap)], sem.at[k, h], f"{name}#k={k}#h={h}")

    def fill(k, h, values):
        made = values.astype(jnp.bfloat16)
        slots_in[k, h, 0:cap] = made[0:cap]
        slots[k, h] = made
        send_near(slots, slots_in, send_sem.at[1], near_sem, k, h)

    if pairs:
        pack_pool(far[0] - 1)
    pack(far[0])
    with jax.named_scope("barrier_wait"):
        pl.semaphore_wait(barrier, len(peers))
    for k in far:
        send(counts, counts_far.at[k], send_sem.at[4], count_sem.at[0], device(k, 0))
    send_far(far[0])
    table = gather_from(0, span)
    for h in range(parts):
        fill(0, h, jnp.dot(table, normed[:, columns(h)], preferred_element_type=jnp.float32))
    for k in sent[1:]:
        if k > 1 and k % 2:
            pack_pool(k - 1)
        pack(k)
        send_far(k)
    def to_column(row, size):
        there = lax.broadcasted_iota(jnp.int32, (size, size), 0)
        here = lax.broadcasted_iota(jnp.int32, (size, size), 1)
        return jnp.sum(jnp.where(there == here, row, 0.0), axis=1, keepdims=True)

    placed_col[...] = to_column(placed_row.astype(jnp.float32), tok_rows).astype(jnp.int32)
    loads[3].wait()
    gate_col[...] = to_column(gate_row_ref[...], tok_rows)

    wait(counts_far.at[pl.ds(1, planes - 1)], count_sem.at[0], "wait_counts")
    sums[...] = counts[...] + jnp.sum(counts_far[pl.ds(1, planes - 1)], axis=0)
    for k, j in near_by:
        send(sums, sums_in.at[j], send_sem.at[5], count_sem.at[1], device(k, j))
    expert = lax.broadcasted_iota(jnp.int32, (lanes, span), 0)
    plane_s, near_s = place_of(expert)
    here = (plane_s == 0) & (expert < n)
    slot = lax.broadcasted_iota(jnp.int32, (lanes, span), 1)
    at_block = ones_at(here & (near_s == slot // cap))
    before_block = ones_at(here & (near_s < slot // cap))
    slot_row = lax.broadcasted_iota(jnp.int32, (1, span), 1)
    rank = (slot_row % cap).astype(jnp.float32)
    for k in far:
        tall = jnp.broadcast_to(counts_far[k], (8, lanes)).astype(jnp.bfloat16)
        held = jnp.dot(tall, at_block, preferred_element_type=jnp.float32)[0:1]
        begin = jnp.dot(tall, before_block, preferred_element_type=jnp.float32)[0:1]
        index = jnp.where(rank < held, begin + rank, -1.0)
        index_row[k] = index.astype(jnp.int32)
        index_col[k] = to_column(index, span).astype(jnp.int32)

    with jax.named_scope("wait_weights"):
        loads[4].wait()
        loads[5].wait()

    def relay(k, h):
        wait(chunk(packed_in, k, h), far_sem.at[k, h], f"wait_far#k={k}#h={h}")
        keep = keep_of(k)
        slot = lax.broadcasted_iota(jnp.int32, (span, keep), 1)
        values = jnp.dot(
            ones_at(slot == index_col[k]), packed_in[k, h, 0:keep],
            preferred_element_type=jnp.float32,
        )
        if k > 1:
            wait(pool_in.at[k, h], pool_sem.at[k, h], f"wait_pool#k={k}#h={h}")
            slot = lax.broadcasted_iota(jnp.int32, (span, pool), 1)
            values += jnp.dot(
                ones_at(slot == pool_row(index_col[k], k)), pool_in[k, h],
                preferred_element_type=jnp.float32,
            )
        fill(k, h, values)
        if k > 1 and k % 2:
            pass_pool(k, h)

    def await_slots(k):
        for h in range(parts):
            wait_near(slots_in, near_sem, k, h, "wait_slots")

    def grow(k):
        @pl.loop(0, first.shape[1] // ff_tile, unroll=min(4, first.shape[1] // ff_tile))
        def _(i):
            part = pl.ds(pl.multiple_of(i * ff_tile, ff_tile), ff_tile)
            grown = jnp.dot(slots_in[k, 0], first[columns(0), part], preferred_element_type=jnp.float32)
            for h in range(1, parts):
                grown += jnp.dot(
                    slots_in[k, h], first[columns(h), part], preferred_element_type=jnp.float32
                )
            hidden[:, part] = jnp.maximum(grown, 0.0).astype(jnp.bfloat16)

    def shrink(k, group):
        for h in group:
            for at in range(0, wide_part, out_tile):
                part = pl.ds(h * wide_part + at, out_tile)
                made = jnp.dot(hidden[...], second[:, part], preferred_element_type=jnp.float32)
                made = made.astype(jnp.bfloat16)
                answers[k, h, :, at : at + out_tile] = made
                answers_in[k, h, 0:cap, at : at + out_tile] = made[0:cap]

    def send_answers(k, h):
        send_near(answers, answers_in, send_sem.at[2], answer_sem, k, h)

    def give_back(k, h):
        wait_near(answers_in, answer_sem, k, h, "wait_answers")
        keep = keep_of(k)
        slot = lax.broadcasted_iota(jnp.int32, (keep, span), 0)
        back[k, h, 0:keep] = jnp.dot(
            ones_at(slot == index_row[k]), answers_in[k, h], preferred_element_type=jnp.float32
        ).astype(jnp.bfloat16)
        send(
            chunk(back, k, h), chunk(back_in, k, h), send_sem.at[3 if k > 1 else 9],
            back_sem.at[k, h], device(k, 0),
        )
        if k > 1:
            slot = lax.broadcasted_iota(jnp.int32, (pool, span), 0)
            values = jnp.dot(
                ones_at(slot == pool_row(index_row[k], k)), answers_in[k, h],
                preferred_element_type=jnp.float32,
            )
            if k % 2 == 0:
                wait(pool_back.at[k + 1, h], merge_sem.at[k + 1, h], f"wait_merge#k={k}#h={h}")
                values += pool_back[k + 1, h].astype(jnp.float32)
            pool_out[k, h] = values.astype(jnp.bfloat16)
            send(
                pool_out.at[k, h], pool_back.at[k, h], send_sem.at[10], merge_sem.at[k, h],
                device(1 if k % 2 else k, 0),
            )

    def picked(k, h):
        if k:
            wait(chunk(back_in, k, h), back_sem.at[k, h], f"wait_back#k={k}#h={h}")
            size, source = keep_of(k), back_in
        else:
            wait_near(answers_in, answer_sem, 0, h, "wait_answers")
            size, source = span, answers_in
        slot = lax.broadcasted_iota(jnp.int32, (tok_rows, size), 1) + k * span
        table = ones_at(slot == placed_col[...])
        values = jnp.dot(table, source[k, h, 0:size], preferred_element_type=jnp.float32)
        if k > 1 and k % 2 == 0:
            wait(pool_back.at[k, h], merge_sem.at[k, h], f"wait_pool_back#k={k}#h={h}")
            slot = lax.broadcasted_iota(jnp.int32, (tok_rows, pool), 1)
            values += jnp.dot(
                in_pool(slot, placed_col[...], k), pool_back[k, h], preferred_element_type=jnp.float32
            )
        return values

    halves = range(parts)
    todo = far[:1] + far[:0:-1]
    await_slots(0)
    grow(0)
    groups = [halves[i : i + parts // 2] for i in range(0, parts, parts // 2)]
    for group in groups:
        shrink(0, group)
    for k in todo[:2]:
        for h in halves:
            relay(k, h)
    for i, k in enumerate(todo):
        await_slots(k)
        grow(k)
        for k2 in todo[i + 1 : i + 2] if i else []:
            for h in halves:
                relay(k2, h)
        for h in halves:
            if i == 1:
                give_back(todo[0], h)
        for group in groups:
            shrink(k, group)
            for h in group:
                send_answers(k, h)
            for h in group:
                if i > 1:
                    give_back(todo[i - 1], h)
    for h in halves:
        give_back(todo[-1], h)
    for h in halves:
        send_answers(0, h)

    wait(sums_in.at[pl.ds(1, per - 1)], count_sem.at[1])
    whole = sums[...] + jnp.sum(sums_in[pl.ds(1, per - 1)], axis=0)
    routed_ref[0] = jnp.sum(jnp.where(lane == me, whole, 0.0)).astype(jnp.int32)
    over_ref[0] = jnp.sum(jnp.where(lane == n, whole, 0.0)).astype(jnp.int32)

    for h in range(parts):
        total[h] = picked(0, h)
    for k in todo[:-1]:
        for h in range(parts):
            total[h] += picked(k, h)
    for h in range(parts):
        found = total[h] + picked(todo[-1], h)
        kept = tokens_ref[:, columns(h)].astype(jnp.float32)
        mixed_ref[:, columns(h)] = (kept + gate_col[...] * found).astype(jnp.bfloat16)
        pltpu.make_async_copy(
            mixed_ref.at[:, columns(h)], mixed_hbm.at[:, columns(h)], store_sem.at[h]
        ).start()

    wait(packed.at[1, :, pl.ds(0, near_keep)], send_sem.at[6])
    wait(back.at[1, :, pl.ds(0, near_keep)], send_sem.at[9])
    if pairs:
        wait(packed.at[pl.ds(2, planes - 2), :, pl.ds(0, main)], send_sem.at[0])
        wait(back.at[pl.ds(2, planes - 2), :, pl.ds(0, main)], send_sem.at[3])
        wait(pooled.at[pl.ds(1, len(pairs))], send_sem.at[7])
        wait(pooled.at[pl.ds(1, len(pairs))], send_sem.at[8])
        wait(pool_out.at[pl.ds(2, planes - 2)], send_sem.at[10])
    wait(slots.at[:, :, pl.ds(cap, span - cap)], send_sem.at[1])
    wait(answers.at[:, :, pl.ds(cap, span - cap)], send_sem.at[2])
    wait(counts_far.at[pl.ds(1, planes - 1)], send_sem.at[4])
    wait(sums_in.at[pl.ds(1, per - 1)], send_sem.at[5])
    for h in halves:
        wait(mixed_ref.at[:, columns(h)], store_sem.at[h])


def packed_layer(rows, cols, tokens, expert_ids, gate_prob, norm_gain, weight_in, weight_out):
    tok_rows, width = tokens.shape
    hidden_width = weight_in.shape[2]
    n = rows * cols
    low = min(2, cols)
    planes = cols // low
    per = n // planes
    cap = 2 * tok_rows // n
    span = per * cap
    near_keep, main, pool = (-(-part * span // 256) * 16 for part in (13, 9, 3))
    parts = 4
    part = width // parts
    lanes = -(-(n + 1) // 128) * 128
    smem = pl.BlockSpec(memory_space=pltpu.SMEM)
    hbm = pl.BlockSpec(memory_space=pl.ANY)
    tight = pltpu.VMEM((planes, parts, near_keep, part), jnp.bfloat16)
    shared = pltpu.VMEM((planes, parts, pool, part), jnp.bfloat16)
    some = pltpu.VMEM((max(1, planes // 2), parts, pool, part), jnp.bfloat16)
    loose = pltpu.VMEM((planes, parts, span, part), jnp.bfloat16)
    each = pltpu.SemaphoreType.DMA((planes, parts))
    return pl.pallas_call(
        functools.partial(
            packed_kernel, rows, cols, low, cap, near_keep, main, pool, parts,
            min(512, hidden_width), min(256, part),
        ),
        out_shape=(
            jax.ShapeDtypeStruct((tok_rows, width), jnp.bfloat16),
            jax.ShapeDtypeStruct((1,), jnp.int32),
            jax.ShapeDtypeStruct((1,), jnp.int32),
        ),
        in_specs=[hbm, hbm, hbm, hbm, hbm, hbm],
        out_specs=(hbm, smem, smem),
        scratch_shapes=[
            pltpu.VMEM((tok_rows, width), jnp.bfloat16),
            pltpu.VMEM((1, tok_rows), jnp.int32),
            pltpu.VMEM((1, tok_rows), jnp.float32),
            pltpu.VMEM((1, width), jnp.float32),
            pltpu.VMEM((tok_rows, width), jnp.bfloat16),
            pltpu.VMEM((width, hidden_width), jnp.bfloat16),
            pltpu.VMEM((hidden_width, width), jnp.bfloat16),
            pltpu.VMEM((tok_rows, width), jnp.bfloat16),
            tight, tight, loose, loose, loose, loose, tight, tight,
            some, shared, shared, shared,
            pltpu.VMEM((span, hidden_width), jnp.bfloat16),
            pltpu.VMEM((parts, tok_rows, part), jnp.float32),
            pltpu.VMEM((1, lanes), jnp.float32),
            pltpu.VMEM((planes, 1, lanes), jnp.float32),
            pltpu.VMEM((1, lanes), jnp.float32),
            pltpu.VMEM((per, 1, lanes), jnp.float32),
            pltpu.VMEM((planes, 1, span), jnp.int32),
            pltpu.VMEM((planes, span, 1), jnp.int32),
            pltpu.VMEM((tok_rows, 1), jnp.int32),
            pltpu.VMEM((tok_rows, 1), jnp.float32),
            pltpu.SemaphoreType.DMA((6,)),
            pltpu.SemaphoreType.DMA((parts,)),
            pltpu.SemaphoreType.DMA((11,)),
            each, each, each, each, each, each,
            pltpu.SemaphoreType.DMA((2,)),
        ],
        compiler_params=pltpu.CompilerParams(
            collective_id=0, has_side_effects=True, vmem_limit_bytes=56 * 1024 * 1024
        ),
    )(
        tokens,
        expert_ids.reshape(1, tok_rows),
        gate_prob.reshape(1, tok_rows),
        norm_gain.reshape(1, width),
        weight_in,
        weight_out,
    )


def slotted_layer(rows, cols, tokens, expert_ids, gate_prob, norm_gain, weight_in, weight_out):
    tok_rows, width = tokens.shape
    hidden_width = weight_in.shape[2]
    n = rows * cols
    cap = 2 * tok_rows // n
    lanes = -(-n // 128) * 128
    per = max(1, min(n, 256 // cap))
    groups = n // per
    vmem = pl.BlockSpec(memory_space=pltpu.VMEM)
    hbm = pl.BlockSpec(memory_space=pl.ANY)
    block = pltpu.VMEM((n, cap, width), jnp.bfloat16)
    back, routed = pl.pallas_call(
        functools.partial(kernel, rows, cols, cap, groups, min(512, hidden_width), min(256, width)),
        out_shape=(
            jax.ShapeDtypeStruct((tok_rows, width), jnp.bfloat16),
            jax.ShapeDtypeStruct((1,), jnp.int32),
        ),
        in_specs=[vmem, vmem, vmem, hbm, hbm],
        out_specs=(vmem, pl.BlockSpec(memory_space=pltpu.SMEM)),
        scratch_shapes=[
            pltpu.VMEM((width, hidden_width), jnp.bfloat16),
            pltpu.VMEM((hidden_width, width), jnp.bfloat16),
            pltpu.VMEM((tok_rows, width), jnp.bfloat16),
            block, block, block, block,
            pltpu.VMEM((per * cap, hidden_width), jnp.bfloat16),
            pltpu.VMEM((tok_rows, width), jnp.float32),
            pltpu.VMEM((1, lanes), jnp.float32),
            pltpu.VMEM((n, 1, lanes), jnp.float32),
            pltpu.VMEM((tok_rows, 1), jnp.int32),
            pltpu.SemaphoreType.DMA((2,)),
            pltpu.SemaphoreType.DMA((3,)),
            pltpu.SemaphoreType.DMA((groups,)),
            pltpu.SemaphoreType.DMA((groups,)),
            pltpu.SemaphoreType.DMA,
        ],
        compiler_params=pltpu.CompilerParams(
            collective_id=1, has_side_effects=True, vmem_limit_bytes=56 * 1024 * 1024
        ),
    )(
        tokens,
        expert_ids.reshape(1, tok_rows),
        norm_gain.reshape(1, width),
        weight_in,
        weight_out,
    )
    wide = tokens.astype(jnp.float32)
    mixed = (wide + gate_prob[:, None] * back.astype(jnp.float32)).astype(jnp.bfloat16)
    return mixed


def on_device(rows, cols, *args):
    mixed, routed, over = packed_layer(rows, cols, *args)
    mixed = lax.cond(
        over[0] > 0, lambda given, *all_args: slotted_layer(rows, cols, *all_args),
        lambda given, *all_args: given, mixed, *args,
    )
    return (mixed, routed)


def solution(mesh):
    return jax.shard_map(
        functools.partial(on_device, mesh.shape["row"], mesh.shape["col"]),
        mesh=mesh,
        in_specs=(
            P(("row", "col"), None),
            P(("row", "col"), None),
            P(("row", "col")),
            P(),
            P(("row", "col"), None, None),
            P(("row", "col"), None, None),
        ),
        out_specs=(P(("row", "col"), None), P(("row", "col"))),
        check_vma=False,
    )
```
